32 devices in a mesh: crop: 1, dap: 32 (over z, y, x, core).
Axes of the slice: x: 2, y: 2, z: 4, core: 2. Of those that a mesh axis runs over, the one named last changes fastest.
Arguments:
- homolog_features: bfloat16 [128, 128, 256], P(('crop', 'dap')), may hold values from -6 to 6
- twofold_features: bfloat16 [128, 128, 128], P(('crop', 'dap')), may hold values from -6 to 6
- twofold_offset_map: bfloat16 [128, 8], replicated, may hold values from -0.5 to 0.5
- horizontal_attend_entry_maps: bfloat16 [256, 1024], replicated, may hold values from -2 to 2
- horizontal_attend_exit_map: bfloat16 [256, 256], replicated, may hold values from -0.375 to 0.375
- vertical_attend_entry_maps: bfloat16 [256, 1024], replicated, may hold values from -2 to 2
- vertical_attend_exit_map: bfloat16 [256, 256], replicated, may hold values from -0.375 to 0.375
- tensor_product_factors: bfloat16 [256, 64], replicated, may hold values from -0.375 to 0.375
- tensor_product_exit_map: bfloat16 [1024, 128], replicated, may hold values from -1 to 1
Outputs:
- alignment_output: bfloat16 [128, 128, 256], P('crop', 'dap')
- pair_output: bfloat16 [128, 128, 128], P(('crop', 'dap'))
The draws below stay inside these ranges and needn't reach their ends.
All inputs are finite; a program needn't handle non-finite values.
Results may differ from the reference program's by a relative error of at most 0.0085.
Values may be sent and summed in bfloat16 or wider, within the bound.
No kernel may reach another device: no remote copies, remote signals or barrier semaphores. Data moves between devices by JAX's collectives and lax.ppermute only.
A program may use at most 64 MiB of HBM per device.

```python
import math
import jax
import jax.numpy as jnp
from jax import lax

FEATURE_DEPTH = 256
CZ = 128
HEAD_NUMBER = 8
HEAD_DEPTH = 32
PRODUCT_SPAN = 32
HOMOLOG_NUMBER = 128
CROP_LENGTH = 128


def attention_weights(key, random_seed_integer):
    random_samples = jax.random.normal(jax.random.fold_in(key, random_seed_integer), (FEATURE_DEPTH, 4 * HEAD_NUMBER * HEAD_DEPTH), jnp.float32)
    random_samples = jnp.clip(random_samples, -6.0, 6.0) / math.sqrt(FEATURE_DEPTH)
    random_samples = jnp.clip(random_samples, -2.0, 2.0)
    return random_samples.astype(jnp.bfloat16)


def draw_horizontal_attend_entry_maps(key, part):
    return attention_weights(key, 11)


def draw_vertical_attend_entry_maps(key, part):
    return attention_weights(key, 23)


def shard_levels(own_key, dims, cuts, least, high):
    gain = 1.0
    for axis_at, blocks in cuts:
        heights = jax.random.uniform(jax.random.fold_in(jax.random.fold_in(own_key, 6), axis_at), (blocks,), jnp.float32, least / len(cuts), high / len(cuts))
        gain = gain * jnp.repeat(jnp.exp(heights), dims[axis_at] // blocks).reshape((-1,) + (1,) * (len(dims) - 1 - axis_at))
    return gain


def scatter_about(own_key, dims, deviation, most, cuts=(), kind=jnp.bfloat16):
    array = jax.random.normal(own_key, dims, jnp.float32) * deviation
    if len(cuts) > 0:
        array = shard_levels(own_key, dims, cuts, -0.22, 0.18) * array
    return jnp.clip(array, min=-most, max=most).astype(kind)


def setup_inputs(seed: int = 0, part: int = 0) -> dict:
    streams_of = jax.random.split(jax.random.key(seed), 10)
    part_splits = jax.random.split(jax.random.fold_in(streams_of[9], part), 10)
    return {
        "homolog_features": scatter_about(part_splits[0], (HOMOLOG_NUMBER, CROP_LENGTH, FEATURE_DEPTH), 1.0, 6.0, ((0, 32),)),
        "twofold_features": scatter_about(part_splits[1], (CROP_LENGTH, CROP_LENGTH, CZ), 1.0, 6.0, ((0, 32),)),
        "twofold_offset_map": scatter_about(streams_of[2], (CZ, HEAD_NUMBER), CZ ** -0.5, 0.5),
        "horizontal_attend_entry_maps": draw_horizontal_attend_entry_maps(jax.random.fold_in(streams_of[9], 71), part),
        "horizontal_attend_exit_map": scatter_about(streams_of[4], (HEAD_NUMBER * HEAD_DEPTH, FEATURE_DEPTH), (HEAD_NUMBER * HEAD_DEPTH) ** -0.5, 0.375),
        "vertical_attend_entry_maps": draw_vertical_attend_entry_maps(jax.random.fold_in(streams_of[9], 71), part),
        "vertical_attend_exit_map": scatter_about(streams_of[6], (HEAD_NUMBER * HEAD_DEPTH, FEATURE_DEPTH), (HEAD_NUMBER * HEAD_DEPTH) ** -0.5, 0.375),
        "tensor_product_factors": scatter_about(streams_of[7], (FEATURE_DEPTH, 2 * PRODUCT_SPAN), FEATURE_DEPTH ** -0.5, 0.375),
        "tensor_product_exit_map": scatter_about(streams_of[8], (PRODUCT_SPAN * PRODUCT_SPAN, CZ), PRODUCT_SPAN ** -0.5, 1.0),
    }


EPSILON = 1e-05

def standardize_features(values):
    values = values.astype(jnp.float32)
    center = values - lax.optimization_barrier(jnp.mean(values, axis=-1, keepdims=True))
    spread = lax.optimization_barrier(jnp.mean(center * center, axis=-1, keepdims=True))
    return center * lax.rsqrt(spread + EPSILON)

def split_heads(packed, head_count):
    pieces = jnp.split(packed, 4, axis=-1)
    return [piece.reshape(piece.shape[:-1] + (head_count, piece.shape[-1] // head_count)) for piece in pieces]

def attend(queries, key_rows, value_rows, gate_rows, pair_bias):
    head_size = queries.shape[-1]
    scores = jnp.einsum('bihd,bjhd->bhij', queries.astype(jnp.float32), key_rows.astype(jnp.float32)) / math.sqrt(head_size)
    scores = scores + pair_bias
    highest = lax.optimization_barrier(jnp.max(scores, axis=-1, keepdims=True))
    expo = jnp.exp(scores - highest)
    weights = (expo / lax.optimization_barrier(jnp.sum(expo, axis=-1, keepdims=True))).astype(jnp.bfloat16)
    attended = jnp.einsum('bhij,bjhd->bihd', weights.astype(jnp.float32), value_rows.astype(jnp.float32))
    gated = (jax.nn.sigmoid(gate_rows.astype(jnp.float32)) * attended).astype(jnp.bfloat16)
    return gated.reshape(gated.shape[:2] + (gated.shape[2] * gated.shape[3],))

def reference(homolog_features, twofold_features, twofold_offset_map, horizontal_attend_entry_maps, horizontal_attend_exit_map, vertical_attend_entry_maps, vertical_attend_exit_map, tensor_product_factors, tensor_product_exit_map):
    head_count = twofold_offset_map.shape[1]
    horizontal_standardized = standardize_features(homolog_features).astype(jnp.bfloat16)
    horizontal_mapped_features = jnp.einsum('src,cf->srf', horizontal_standardized.astype(jnp.float32), horizontal_attend_entry_maps.astype(jnp.float32)).astype(jnp.bfloat16)
    pair_norm = standardize_features(twofold_features).astype(jnp.bfloat16)
    pair_bias = jnp.einsum('ijz,zh->hij', pair_norm.astype(jnp.float32), twofold_offset_map.astype(jnp.float32)).astype(jnp.bfloat16)
    bias_wide = pair_bias.astype(jnp.float32)[None]
    heads_row = split_heads(horizontal_mapped_features, head_count)

    def one_sequence(items):
        return attend(items[0][None], items[1][None], items[2][None], items[3][None], bias_wide)[0]
    horizontal_sigmoid_scaled = lax.map(one_sequence, tuple(heads_row))
    homolog_line = (homolog_features.astype(jnp.float32) + jnp.einsum('asd,dy->asy', horizontal_sigmoid_scaled.astype(jnp.float32), horizontal_attend_exit_map.astype(jnp.float32))).astype(jnp.bfloat16)
    column_layer_norm = standardize_features(homolog_line).astype(jnp.bfloat16)
    col_proj = jnp.einsum('src,cf->rsf', column_layer_norm.astype(jnp.float32), vertical_attend_entry_maps.astype(jnp.float32)).astype(jnp.bfloat16)
    heads_col = split_heads(col_proj, head_count)

    def one_residue(items):
        return attend(items[0][None], items[1][None], items[2][None], items[3][None], 0.0)[0]
    column_gated_output = lax.map(one_residue, tuple(heads_col))
    alignment_output = (homolog_line.astype(jnp.float32) + jnp.einsum('ihb,by->hiy', column_gated_output.astype(jnp.float32), vertical_attend_exit_map.astype(jnp.float32))).astype(jnp.bfloat16)
    outer_width = tensor_product_factors.shape[1] // 2
    outer_layer_norm = standardize_features(alignment_output).astype(jnp.bfloat16).astype(jnp.float32)
    left = jnp.einsum('src,cf->rsf', outer_layer_norm, tensor_product_factors[:, :outer_width].astype(jnp.float32)).astype(jnp.bfloat16)
    right = jnp.einsum('src,cf->rsf', outer_layer_norm, tensor_product_factors[:, outer_width:].astype(jnp.float32)).astype(jnp.bfloat16)
    right_wide = right.astype(jnp.float32)
    homolog_tally = homolog_features.shape[0]

    def one_row(items):
        left_row, pair_row = items
        product = jnp.einsum('sc,jse->jce', left_row.astype(jnp.float32), right_wide) / homolog_tally
        flat = product.astype(jnp.bfloat16).reshape(product.shape[0], outer_width * outer_width)
        residual_delta = jnp.dot(flat, tensor_product_exit_map, preferred_element_type=jnp.float32)
        return (pair_row.astype(jnp.float32) + residual_delta).astype(jnp.bfloat16)
    pair_output = lax.map(one_row, (left, twofold_features))
    return (alignment_output, pair_output)
```

```python
import math

import jax
import jax.numpy as jnp
from jax import lax
from jax.sharding import PartitionSpec as P

EPSILON = 1e-05


def standardize_features(values):
    values = values.astype(jnp.float32)
    center = values - jnp.mean(values, axis=-1, keepdims=True)
    spread = jnp.mean(center * center, axis=-1, keepdims=True)
    return center * lax.rsqrt(spread + EPSILON)


def split_heads(packed, head_count):
    pieces = jnp.split(packed, 4, axis=-1)
    return [
        piece.reshape(piece.shape[:-1] + (head_count, piece.shape[-1] // head_count))
        for piece in pieces
    ]


def attend(queries, key_rows, value_rows, gate_rows, pair_bias):
    head_size = queries.shape[-1]
    scores = jnp.einsum(
        "bihd,bjhd->bhij", queries, key_rows, preferred_element_type=jnp.float32
    ) / math.sqrt(head_size)
    scores = scores + pair_bias
    highest = jnp.max(scores, axis=-1, keepdims=True)
    expo = jnp.exp(scores - highest)
    weights = (expo / jnp.sum(expo, axis=-1, keepdims=True)).astype(jnp.bfloat16)
    attended = jnp.einsum(
        "bhij,bjhd->bihd", weights, value_rows, preferred_element_type=jnp.float32
    )
    gated = (jax.nn.sigmoid(gate_rows.astype(jnp.float32)) * attended).astype(jnp.bfloat16)
    return gated.reshape(gated.shape[:2] + (gated.shape[2] * gated.shape[3],))


def mapped_horizontal_piece(homolog_features, horizontal_attend_entry_maps):
    horizontal_standardized = standardize_features(homolog_features).astype(jnp.bfloat16)
    return jnp.einsum(
        "src,cf->srf",
        horizontal_standardized,
        horizontal_attend_entry_maps,
        preferred_element_type=jnp.float32,
    ).astype(jnp.bfloat16)


def collect_bias(twofold_features, twofold_offset_map):
    pair_norm = standardize_features(twofold_features).astype(jnp.bfloat16)
    local_bias = jnp.einsum(
        "ijz,zh->hij", pair_norm, twofold_offset_map, preferred_element_type=jnp.float32
    ).astype(jnp.bfloat16)
    width = lax.axis_size("dap")
    heads, rows, residues = local_bias.shape
    copies = jnp.broadcast_to(local_bias[None], (width, heads, rows, residues))
    blocks = lax.all_to_all(copies, "dap", split_axis=0, concat_axis=0, tiled=True)
    return blocks.transpose(1, 0, 2, 3).reshape(heads, width * rows, residues)


def gather_rounds(width):
    rounds = []
    stride = width
    while stride > 1:
        radix = 4 if stride % 4 == 0 else 2
        stride //= radix
        rounds.append([step * stride for step in range(1, radix)])
    return rounds


def gather_blocks(block):
    width = lax.axis_size("dap")
    if width & (width - 1):
        return lax.all_gather(block, "dap", axis=0)
    stacked = block[None]
    order = [0]
    for steps in gather_rounds(width):
        arrived = [
            lax.ppermute(stacked, "dap", [(d, d ^ step) for d in range(width)])
            for step in steps
        ]
        stacked = jnp.concatenate([stacked, *arrived], axis=0)
        order = order + [k ^ step for step in steps for k in order]
    place = [order.index(k) for k in range(width)]
    index = jnp.asarray(place, jnp.int32)[jnp.arange(width) ^ lax.axis_index("dap")]
    return jnp.take(stacked, index, axis=0)


def column_delta(received_blocks, vertical_attend_entry_maps, vertical_attend_exit_map, head_count):
    column_alignment = received_blocks[:, 0]
    column_layer_norm = standardize_features(column_alignment).astype(jnp.bfloat16)
    col_proj = jnp.einsum(
        "skc,cf->ksf",
        column_layer_norm,
        vertical_attend_entry_maps,
        preferred_element_type=jnp.float32,
    ).astype(jnp.bfloat16)
    queries, key_rows, value_rows, gate_rows = split_heads(col_proj, head_count)
    column_gated_output = attend(queries, key_rows, value_rows, gate_rows, 0.0)
    residual_delta = jnp.einsum(
        "ksf,fc->skc",
        column_gated_output,
        vertical_attend_exit_map,
        preferred_element_type=jnp.float32,
    )
    return (column_alignment.astype(jnp.float32) + residual_delta).astype(jnp.bfloat16)


def per_device(
    homolog_features,
    twofold_features,
    twofold_offset_map,
    horizontal_attend_entry_maps,
    horizontal_attend_exit_map,
    vertical_attend_entry_maps,
    vertical_attend_exit_map,
    tensor_product_factors,
    tensor_product_exit_map,
):
    head_count = twofold_offset_map.shape[1]
    horizontal_mapped_features = mapped_horizontal_piece(
        homolog_features, horizontal_attend_entry_maps
    )
    gathered = collect_bias(twofold_features, twofold_offset_map)
    bias_wide = gathered.astype(jnp.float32)[None]
    heads_row = split_heads(horizontal_mapped_features, head_count)

    def one_sequence(items):
        return attend(items[0][None], items[1][None], items[2][None], items[3][None], bias_wide)[0]

    horizontal_sigmoid_scaled = lax.map(one_sequence, tuple(heads_row))
    homolog_line = (
        homolog_features.astype(jnp.float32)
        + jnp.einsum(
            "asd,dy->asy",
            horizontal_sigmoid_scaled,
            horizontal_attend_exit_map,
            preferred_element_type=jnp.float32,
        )
    ).astype(jnp.bfloat16)
    parallel_width = lax.axis_size("dap")
    sequence_local, residue_total, channel_count = homolog_line.shape
    alignment_blocks = homolog_line.reshape(
        sequence_local, parallel_width, residue_total // parallel_width, channel_count
    )
    alignment_output = column_delta(
        lax.all_to_all(alignment_blocks, "dap", split_axis=1, concat_axis=0, tiled=True),
        vertical_attend_entry_maps,
        vertical_attend_exit_map,
        head_count,
    )
    outer_width = tensor_product_factors.shape[1] // 2
    homolog_tally = alignment_output.shape[0]
    residue_local = alignment_output.shape[1]
    outer_layer_norm = standardize_features(alignment_output).astype(jnp.bfloat16)
    left_rows = jnp.einsum(
        "src,cf->rsf",
        outer_layer_norm,
        tensor_product_factors[:, :outer_width],
        preferred_element_type=jnp.float32,
    ).astype(jnp.bfloat16)
    right_rows = jnp.einsum(
        "src,cf->rsf",
        outer_layer_norm,
        tensor_product_factors[:, outer_width:],
        preferred_element_type=jnp.float32,
    ).astype(jnp.bfloat16)
    right_flat = right_rows.reshape(residue_local, homolog_tally * outer_width)
    segment = gather_blocks(right_flat)
    segment = segment.reshape(segment.shape[0] * segment.shape[1], segment.shape[2])
    count_rows = segment.shape[0]
    right_three = segment.reshape(count_rows, homolog_tally, outer_width)
    product = (
        jnp.einsum("isc,jse->ijce", left_rows, right_three, preferred_element_type=jnp.float32)
        / homolog_tally
    )
    flat = product.astype(jnp.bfloat16).reshape(
        residue_local * count_rows, outer_width * outer_width
    )
    residual_delta = jnp.dot(flat, tensor_product_exit_map, preferred_element_type=jnp.float32)
    residual_delta = residual_delta.reshape(residue_local, count_rows, residual_delta.shape[-1])
    base_rows = twofold_features.astype(jnp.float32)
    pair_output = (base_rows + residual_delta).astype(jnp.bfloat16)
    return (alignment_output, pair_output)


def solution(mesh):
    in_specs = (
        P(("crop", "dap"), None, None),
        P(("crop", "dap"), None, None),
        P(),
        P(),
        P(),
        P(),
        P(),
        P(),
        P(),
    )
    out_specs = (P("crop", "dap", None), P(("crop", "dap"), None, None))
    return jax.shard_map(
        per_device, mesh=mesh, in_specs=in_specs, out_specs=out_specs, check_vma=False
    )
```

```python
import functools
import math

import jax
import jax.numpy as jnp
from jax import lax
from jax.experimental import pallas as pl
from jax.experimental.pallas import tpu as pltpu
from jax.sharding import PartitionSpec as P

EPSILON = 1e-05
LANES = 128
F32 = jnp.float32
BF16 = jnp.bfloat16
VMEM = pl.BlockSpec(memory_space=pltpu.VMEM)
SMEM = pl.BlockSpec(memory_space=pltpu.SMEM)


def standardize(values):
    center = values - jnp.mean(values, axis=-1, keepdims=True)
    spread = jnp.mean(center * center, axis=-1, keepdims=True)
    return (center * lax.rsqrt(spread + EPSILON)).astype(BF16)


def dot(left, right):
    return jnp.dot(left, right, preferred_element_type=F32)


def dot_t(left, right):
    return lax.dot_general(left, right, (((1,), (1,)), ((), ())), preferred_element_type=F32)


def call(body, out_shape, scratch=(), in_specs=None, count=0, flops=0):
    many = isinstance(out_shape, (tuple, list))
    return pl.pallas_call(
        body,
        out_shape=out_shape,
        in_specs=in_specs or [VMEM] * count,
        out_specs=[VMEM] * len(out_shape) if many else VMEM,
        scratch_shapes=list(scratch),
        cost_estimate=pl.CostEstimate(flops=flops, bytes_accessed=0, transcendentals=0),
    )


def lane_masks(width, rows):
    lane = lax.broadcasted_iota(jnp.int32, (rows, LANES), 1)
    return [
        (lane >= start) & (lane < start + width) for start in range(0, LANES, width)
    ]


def masked_rows(block, masks):
    zero = jnp.zeros_like(block)
    return jnp.concatenate([jnp.where(mask, block, zero) for mask in masks], axis=0)


def bias_body(pair_ref, map_ref, out_ref, *, copies):
    rows, _, _ = pair_ref.shape
    heads = map_ref.shape[1]
    height = heads * rows
    row = lax.broadcasted_iota(jnp.int32, (height, heads), 0)
    head = lax.broadcasted_iota(jnp.int32, (height, heads), 1)
    total = None
    for at in range(rows):
        spread = jnp.where(row == head * rows + at, 1.0, 0.0).astype(BF16)
        weights = dot_t(spread, map_ref[...]).astype(BF16)
        part = dot_t(weights, standardize(pair_ref[at].astype(F32)))
        total = part if total is None else total + part
    block = total.astype(BF16)
    for copy in range(copies):
        out_ref[copy * height : (copy + 1) * height, :] = block


def scores_of(proj, head_size, masks):
    width = proj.shape[1] // 4
    scale = 1.0 / math.sqrt(head_size)
    scores = []
    for start in range(0, width, LANES):
        queries = proj[:, start : start + LANES]
        keys = masked_rows(proj[:, width + start : width + start + LANES], masks)
        scores.append(dot_t(queries, keys) * scale)
    return scores


def attended_of(scores, values, gates, masks):
    keys = values.shape[0]
    pieces = []
    for at in range(len(masks)):
        piece = scores[at]
        highest = jnp.max(piece, axis=-1, keepdims=True)
        pieces.append(jnp.exp(piece - highest).astype(BF16))
    ones = jnp.ones((keys, LANES), BF16)
    table = jnp.concatenate([masked_rows(values, masks), masked_rows(ones, masks)], axis=1)
    sums = dot(jnp.concatenate(pieces, axis=1), table)
    gate = jax.nn.sigmoid(gates.astype(F32))
    return (gate * (sums[:, :LANES] / sums[:, LANES:])).astype(BF16)


def row_scores_body(features_ref, maps_ref, proj_ref, scores_ref, *, head_size):
    sequences, residues, _ = features_ref.shape
    masks = lane_masks(head_size, residues)
    for at in range(sequences):
        normal = standardize(features_ref[at].astype(F32))
        proj = dot(normal, maps_ref[...]).astype(BF16)
        proj_ref[at] = proj
        for block, scores in enumerate(scores_of(proj, head_size, masks)):
            scores_ref[at, block] = scores


def row_body(
    bias_ref, proj_ref, scores_ref, features_ref, exit_ref, out_ref, wide, bias, sent, *, blocks, heads, head_size
):
    sequences, residues, channels = features_ref.shape
    rows = residues // blocks
    wide[...] = bias_ref[...].astype(F32)
    for source in range(blocks):
        for head in range(heads):
            start = (source * heads + head) * rows
            bias[head, source * rows : (source + 1) * rows, :] = wide[start : start + rows, :]
    masks = lane_masks(head_size, residues)
    for at in range(sequences):
        gated = []
        for block, start in enumerate(range(0, channels, LANES)):
            scores = [
                scores_ref[at, block, :, k * residues : (k + 1) * residues]
                + bias[block * len(masks) + k]
                for k in range(len(masks))
            ]
            values = proj_ref[at, :, 2 * channels + start : 2 * channels + start + LANES]
            gates = proj_ref[at, :, 3 * channels + start : 3 * channels + start + LANES]
            gated.append(attended_of(scores, values, gates, masks))
        line = features_ref[at].astype(F32) + dot(jnp.concatenate(gated, axis=1), exit_ref[...])
        for target in range(blocks):
            start = (target * sequences + at) * rows
            sent[start : start + rows, :] = line[target * rows : (target + 1) * rows, :]
    out_ref[...] = sent[...].astype(BF16)


def column_body(
    received_ref, maps_ref, exit_ref, factors_ref, out_ref, left_ref, right_ref, wide, done, *, rows, head_size
):
    total, channels = received_ref.shape
    sequences = total // rows
    span = factors_ref.shape[0] // 2
    tiles = range(channels // LANES)
    for tile in tiles:
        wide[tile] = received_ref[:, tile * LANES : (tile + 1) * LANES].astype(F32)
    if left_ref.shape[0] > rows * span:
        left_ref[...] = jnp.zeros_like(left_ref)
    masks = lane_masks(head_size, sequences)
    for at in range(rows):
        chosen = pl.ds(at, sequences, stride=rows)
        line = jnp.concatenate([wide[tile, chosen, :] for tile in tiles], axis=1)
        proj = dot(standardize(line), maps_ref[...]).astype(BF16)
        gated = []
        for block, scores in enumerate(scores_of(proj, head_size, masks)):
            start = block * LANES
            pieces = [scores[:, k * sequences : (k + 1) * sequences] for k in range(len(masks))]
            values = proj[:, 2 * channels + start : 2 * channels + start + LANES]
            gates = proj[:, 3 * channels + start : 3 * channels + start + LANES]
            gated.append(attended_of(pieces, values, gates, masks))
        line = line + dot(jnp.concatenate(gated, axis=1), exit_ref[...])
        line = line.astype(BF16).astype(F32)
        for tile in tiles:
            done[tile, chosen, :] = line[:, tile * LANES : (tile + 1) * LANES]
        factors = dot_t(factors_ref[...], standardize(line)).astype(BF16)
        left_ref[at * span : (at + 1) * span, :] = factors[:span]
        right_ref[at * span : (at + 1) * span, :] = factors[span:]
    for tile in tiles:
        out_ref[:, tile * LANES : (tile + 1) * LANES] = done[tile].astype(BF16)


def outer_body(
    me_ref, left_ref, *refs, order, span, count
):
    right_refs = refs[: -6]
    pair_ref, exit_ref, out_ref, product, lhs, rhs = refs[-6:]
    rows, residues, depth = pair_ref.shape
    width = rows * span
    lanes = left_ref.shape[0]
    scale = 1.0 / count
    at = 0
    for right_ref in right_refs:
        for block in range(right_ref.shape[0] // width):
            source = jnp.bitwise_xor(me_ref[0], order[at])
            start = pl.multiple_of(source * width, width)
            product[pl.ds(start, width), :] = (
                dot_t(right_ref[block * width : (block + 1) * width, :], left_ref[...]) * scale
            )
            at += 1
    pairs = rows // 2
    lane = lax.broadcasted_iota(jnp.int32, (residues, lanes), 1)
    zero = jnp.zeros((span, depth), BF16)
    for e in range(span):
        part = product[pl.ds(e, residues, stride=span), :]
        for pair in range(pairs):
            start = pair * 2 * span
            keep = part if pairs == 1 else jnp.where((lane >= start) & (lane < start + 2 * span), part, 0.0)
            lhs[pair * residues : (pair + 1) * residues, e * lanes : (e + 1) * lanes] = keep.astype(BF16)
        weights = exit_ref[e * span : (e + 1) * span, :]
        for row in range(rows):
            side = [weights, zero] if row % 2 == 0 else [zero, weights]
            start = e * lanes + row * span
            rhs[start : start + span, :] = jnp.concatenate(side, axis=1)
        if lanes > width:
            start = e * lanes + width
            rhs[start : start + lanes - width, :] = jnp.zeros((lanes - width, 2 * depth), BF16)
    delta = dot(lhs[...], rhs[...])
    for row in range(rows):
        start = (row // 2) * residues
        out_ref[row] = (
            pair_ref[row].astype(F32)
            + delta[start : start + residues, (row % 2) * depth : (row % 2 + 1) * depth]
        ).astype(BF16)


def gather_rounds(width):
    rounds = []
    stride = width
    while stride > 1:
        radix = 4 if stride % 4 == 0 else 2
        stride //= radix
        rounds.append([step * stride for step in range(1, radix)])
    return rounds


def gather_blocks(block):
    width = lax.axis_size("dap")
    pieces = [block]
    order = [0]
    for steps in gather_rounds(width):
        stacked = jnp.concatenate(pieces, axis=0) if len(pieces) > 1 else pieces[0]
        pieces = [stacked] + [
            lax.ppermute(stacked, "dap", [(d, d ^ step) for d in range(width)])
            for step in steps
        ]
        order = order + [k ^ step for step in steps for k in order]
    return pieces, order


def per_device(
    homolog_features,
    twofold_features,
    twofold_offset_map,
    horizontal_attend_entry_maps,
    horizontal_attend_exit_map,
    vertical_attend_entry_maps,
    vertical_attend_exit_map,
    tensor_product_factors,
    tensor_product_exit_map,
):
    width = lax.axis_size("dap")
    sequences, residues, channels = homolog_features.shape
    rows, _, depth = twofold_features.shape
    heads = twofold_offset_map.shape[1]
    head_size = channels // heads
    groups = channels // LANES
    span = tensor_product_factors.shape[1] // 2
    count = sequences * width
    lanes = max(rows * span, LANES)
    struct = jax.ShapeDtypeStruct

    copies = call(
        functools.partial(bias_body, copies=width),
        struct((width * heads * rows, residues), BF16),
        count=2,
    )(twofold_features, twofold_offset_map)
    bias = lax.all_to_all(copies, "dap", split_axis=0, concat_axis=0, tiled=True)
    proj, scores = call(
        functools.partial(row_scores_body, head_size=head_size),
        (
            struct((sequences, residues, 4 * channels), BF16),
            struct((sequences, groups, residues, LANES // head_size * residues), F32),
        ),
        count=2,
        flops=10**9,
    )(homolog_features, horizontal_attend_entry_maps)
    sent = call(
        functools.partial(row_body, blocks=width, heads=heads, head_size=head_size),
        struct((sequences * residues, channels), BF16),
        scratch=[
            pltpu.VMEM((width * heads * rows, residues), F32),
            pltpu.VMEM((heads, residues, residues), F32),
            pltpu.VMEM((sequences * residues, channels), F32),
        ],
        count=5,
    )(bias, proj, scores, homolog_features, horizontal_attend_exit_map)
    received = lax.all_to_all(sent, "dap", split_axis=0, concat_axis=0, tiled=True)
    alignment, left, right = call(
        functools.partial(column_body, rows=rows, head_size=head_size),
        (
            struct((count * rows, channels), BF16),
            struct((lanes, count), BF16),
            struct((rows * span, count), BF16),
        ),
        scratch=[pltpu.VMEM((groups, count * rows, LANES), F32)] * 2,
        count=4,
    )(received, vertical_attend_entry_maps, vertical_attend_exit_map, tensor_product_factors.T)
    pieces, order = gather_blocks(right)
    exit_rows = tensor_product_exit_map.reshape(span, span, depth).transpose(1, 0, 2)
    pair_output = call(
        functools.partial(outer_body, order=tuple(order), span=span, count=count),
        struct(twofold_features.shape, BF16),
        scratch=[
            pltpu.VMEM((span * residues, lanes), F32),
            pltpu.VMEM((rows // 2 * residues, span * lanes), BF16),
            pltpu.VMEM((span * lanes, 2 * depth), BF16),
        ],
        in_specs=[SMEM] + [VMEM] * (len(pieces) + 3),
    )(
        lax.axis_index("dap").astype(jnp.int32).reshape(1),
        left,
        *pieces,
        twofold_features,
        exit_rows.reshape(span * span, depth),
    )
    return (alignment.reshape(count, rows, channels), pair_output)


def solution(mesh):
    in_specs = (
        P(("crop", "dap"), None, None),
        P(("crop", "dap"), None, None),
        P(),
        P(),
        P(),
        P(),
        P(),
        P(),
        P(),
    )
    out_specs = (P("crop", "dap", None), P(("crop", "dap"), None, None))
    return jax.shard_map(
        per_device, mesh=mesh, in_specs=in_specs, out_specs=out_specs, check_vma=False
    )
```

```python
import functools
import math

import jax
import jax.numpy as jnp
from jax import lax
from jax.experimental import pallas as pl
from jax.experimental.pallas import tpu as pltpu
from jax.sharding import PartitionSpec as P

EPSILON = 1e-05
LANES = 128
F32 = jnp.float32
BF16 = jnp.bfloat16
VMEM = pl.BlockSpec(memory_space=pltpu.VMEM)
SMEM = pl.BlockSpec(memory_space=pltpu.SMEM)


def standardize(values):
    center = values - jnp.mean(values, axis=-1, keepdims=True)
    spread = jnp.mean(center * center, axis=-1, keepdims=True)
    return (center * lax.rsqrt(spread + EPSILON)).astype(BF16)


def dot(left, right):
    return jnp.dot(left, right, preferred_element_type=F32)


def dot_t(left, right):
    return lax.dot_general(left, right, (((1,), (1,)), ((), ())), preferred_element_type=F32)


def call(body, out_shapes, args, scratch=(), limit=16 << 20, flops=0):
    scalars = [jnp.issubdtype(arg.dtype, jnp.integer) for arg in args]
    return pl.pallas_call(
        body,
        out_shape=[
            pltpu.VMEM(shape, dtype) if near else jax.ShapeDtypeStruct(shape, dtype)
            for shape, dtype, near in out_shapes
        ],
        in_specs=[SMEM if scalar else VMEM for scalar in scalars],
        out_specs=[VMEM] * len(out_shapes),
        scratch_shapes=list(scratch),
        cost_estimate=pl.CostEstimate(flops=flops, bytes_accessed=0, transcendentals=0),
        compiler_params=pltpu.CompilerParams(vmem_limit_bytes=limit),
    )(*[
        arg if scalar else pltpu.with_memory_space_constraint(arg, pltpu.VMEM)
        for arg, scalar in zip(args, scalars)
    ])


def lane_masks(width, rows):
    lane = lax.broadcasted_iota(jnp.int32, (rows, LANES), 1)
    return [
        (lane >= start) & (lane < start + width) for start in range(0, LANES, width)
    ]


def masked_rows(block, masks):
    zero = jnp.zeros_like(block)
    return jnp.concatenate([jnp.where(mask, block, zero) for mask in masks], axis=0)


def bias_body(pair_ref, map_ref, out_ref, *, copies):
    rows, _, _ = pair_ref.shape
    heads = map_ref.shape[0]
    height = heads * rows
    row = lax.broadcasted_iota(jnp.int32, (height, heads), 0)
    head = lax.broadcasted_iota(jnp.int32, (height, heads), 1)
    total = None
    for at in range(rows):
        spread = jnp.where(row == head * rows + at, 1.0, 0.0).astype(BF16)
        weights = dot(spread, map_ref[...]).astype(BF16)
        part = dot_t(weights, standardize(pair_ref[at].astype(F32)))
        total = part if total is None else total + part
    block = total.astype(BF16)
    for copy in range(copies):
        out_ref[copy * height : (copy + 1) * height, :] = block


def scores_of(proj, head_size, masks):
    width = proj.shape[1] // 4
    scale = 1.0 / math.sqrt(head_size)
    scores = []
    for start in range(0, width, LANES):
        queries = proj[:, start : start + LANES]
        keys = masked_rows(proj[:, width + start : width + start + LANES], masks)
        scores.append(dot_t(queries, keys) * scale)
    return scores


def attended_of(scores, values, gates, masks):
    keys = values.shape[0]
    pieces = []
    for at in range(len(masks)):
        piece = scores[at]
        highest = jnp.max(piece, axis=-1, keepdims=True)
        pieces.append(jnp.exp(piece - highest).astype(BF16))
    ones = jnp.ones((keys, LANES), BF16)
    table = jnp.concatenate([masked_rows(values, masks), masked_rows(ones, masks)], axis=1)
    sums = dot(jnp.concatenate(pieces, axis=1), table)
    gate = jax.nn.sigmoid(gates.astype(F32))
    return (gate * (sums[:, :LANES] / sums[:, LANES:])).astype(BF16)


def row_scores_body(features_ref, maps_ref, proj_ref, scores_ref, *, head_size):
    sequences, residues, _ = features_ref.shape
    masks = lane_masks(head_size, residues)
    for at in range(sequences):
        normal = standardize(features_ref[at].astype(F32))
        proj = dot(normal, maps_ref[...]).astype(BF16)
        proj_ref[at, :, : proj.shape[1]] = proj
        proj_ref[at, :, proj.shape[1] :] = features_ref[at]
        for block, scores in enumerate(scores_of(proj, head_size, masks)):
            scores_ref[at, block] = scores


def row_body(
    bias_ref, proj_ref, scores_ref, exit_ref, out_ref, wide, bias, sent, *, blocks, heads, head_size
):
    sequences, residues, channels = proj_ref.shape
    channels //= 5
    rows = residues // blocks
    wide[...] = bias_ref[...].astype(F32)
    for source in range(blocks):
        for head in range(heads):
            start = (source * heads + head) * rows
            bias[head, source * rows : (source + 1) * rows, :] = wide[start : start + rows, :]
    masks = lane_masks(head_size, residues)
    for at in range(sequences):
        gated = []
        for block, start in enumerate(range(0, channels, LANES)):
            scores = [
                scores_ref[at, block, :, k * residues : (k + 1) * residues]
                + bias[block * len(masks) + k]
                for k in range(len(masks))
            ]
            values = proj_ref[at, :, 2 * channels + start : 2 * channels + start + LANES]
            gates = proj_ref[at, :, 3 * channels + start : 3 * channels + start + LANES]
            gated.append(attended_of(scores, values, gates, masks))
        line = proj_ref[at, :, 4 * channels :].astype(F32) + dot(jnp.concatenate(gated, axis=1), exit_ref[...])
        for target in range(blocks):
            for tile in range(channels // LANES):
                start = ((target * sequences + at) * (channels // LANES) + tile) * rows
                sent[start : start + rows, :] = line[
                    target * rows : (target + 1) * rows, tile * LANES : (tile + 1) * LANES
                ]
    out_ref[...] = sent[...].astype(BF16)


def column_body(
    received_ref, maps_ref, exit_ref, factors_ref, out_ref, left_ref, right_ref, wide, done, *, rows, head_size
):
    channels = maps_ref.shape[0]
    tiles = channels // LANES
    sequences = received_ref.shape[0] // (rows * tiles)
    span = factors_ref.shape[0] // 2
    wide[...] = received_ref[...].astype(F32)
    if left_ref.shape[0] > rows * span:
        left_ref[...] = jnp.zeros_like(left_ref)
    masks = lane_masks(head_size, sequences)
    for at in range(rows):
        chosen = [pl.ds(tile * rows + at, sequences, stride=tiles * rows) for tile in range(tiles)]
        line = jnp.concatenate([wide[rows_of, :] for rows_of in chosen], axis=1)
        proj = dot(standardize(line), maps_ref[...]).astype(BF16)
        gated = []
        for block, scores in enumerate(scores_of(proj, head_size, masks)):
            start = block * LANES
            pieces = [scores[:, k * sequences : (k + 1) * sequences] for k in range(len(masks))]
            values = proj[:, 2 * channels + start : 2 * channels + start + LANES]
            gates = proj[:, 3 * channels + start : 3 * channels + start + LANES]
            gated.append(attended_of(pieces, values, gates, masks))
        line = line + dot(jnp.concatenate(gated, axis=1), exit_ref[...])
        line = line.astype(BF16).astype(F32)
        for tile, rows_of in enumerate(chosen):
            done[rows_of, :] = line[:, tile * LANES : (tile + 1) * LANES]
        factors = dot_t(factors_ref[...], standardize(line)).astype(BF16)
        left_ref[at * span : (at + 1) * span, :] = factors[:span]
        right_ref[at * span : (at + 1) * span, :] = factors[span:]
    out_ref[...] = done[...].astype(BF16)


def table_body(exit_ref, out_ref, wide, *, rows, lanes):
    depth = exit_ref.shape[1]
    span = out_ref.shape[0] // lanes
    wide[...] = exit_ref[...].astype(F32)
    zero = jnp.zeros((span, depth), BF16)
    for e in range(span):
        weights = wide[pl.ds(e, span, stride=span), :].astype(BF16)
        for row in range(rows):
            start = e * lanes + row * span
            side = [weights, zero] if row % 2 == 0 else [zero, weights]
            out_ref[start : start + span, :] = jnp.concatenate(side, axis=1)
        if lanes > rows * span:
            start = e * lanes + rows * span
            out_ref[start : (e + 1) * lanes, :] = jnp.zeros((lanes - rows * span, 2 * depth), BF16)


def outer_body(me_ref, left_ref, *refs, order, span, count):
    right_refs = refs[:-5]
    pair_ref, table_ref, out_ref, product, lhs = refs[-5:]
    rows, residues, depth = pair_ref.shape
    width = rows * span
    lanes = left_ref.shape[0]
    scale = 1.0 / count
    at = 0
    for right_ref in right_refs:
        for block in range(right_ref.shape[0] // width):
            source = jnp.bitwise_xor(me_ref[0], order[at])
            start = pl.multiple_of(source * width, width)
            product[pl.ds(start, width), :] = (
                dot_t(right_ref[block * width : (block + 1) * width, :], left_ref[...]) * scale
            )
            at += 1
    pairs = rows // 2
    lane = lax.broadcasted_iota(jnp.int32, (residues, lanes), 1)
    for e in range(span):
        part = product[pl.ds(e, residues, stride=span), :]
        for pair in range(pairs):
            start = pair * 2 * span
            keep = part if pairs == 1 else jnp.where((lane >= start) & (lane < start + 2 * span), part, 0.0)
            lhs[pair * residues : (pair + 1) * residues, e * lanes : (e + 1) * lanes] = keep.astype(BF16)
    delta = dot(lhs[...], table_ref[...])
    for row in range(rows):
        start = (row // 2) * residues
        out_ref[row] = (
            pair_ref[row].astype(F32)
            + delta[start : start + residues, (row % 2) * depth : (row % 2 + 1) * depth]
        ).astype(BF16)


def gather_rounds(width):
    rounds = []
    stride = width
    while stride > 1:
        radix = 4 if stride % 4 == 0 else 2
        stride //= radix
        rounds.append([step * stride for step in range(1, radix)])
    return rounds


def gather_blocks(block):
    width = lax.axis_size("dap")
    pieces = [block]
    order = [0]
    for steps in gather_rounds(width):
        stacked = jnp.concatenate(pieces, axis=0) if len(pieces) > 1 else pieces[0]
        pieces = [stacked] + [
            lax.ppermute(stacked, "dap", [(d, d ^ step) for d in range(width)])
            for step in steps
        ]
        order = order + [k ^ step for step in steps for k in order]
    return pieces, order


def per_device(
    homolog_features,
    twofold_features,
    twofold_offset_map,
    horizontal_attend_entry_maps,
    horizontal_attend_exit_map,
    vertical_attend_entry_maps,
    vertical_attend_exit_map,
    tensor_product_factors,
    tensor_product_exit_map,
):
    width = lax.axis_size("dap")
    sequences, residues, channels = homolog_features.shape
    rows, _, depth = twofold_features.shape
    heads = twofold_offset_map.shape[1]
    head_size = channels // heads
    groups = channels // LANES
    span = tensor_product_factors.shape[1] // 2
    count = sequences * width
    lanes = max(rows * span, LANES)
    tiles = channels // LANES

    [copies] = call(
        functools.partial(bias_body, copies=width),
        [((width * heads * rows, residues), BF16, False)],
        [twofold_features, twofold_offset_map.T],
    )
    bias = lax.all_to_all(copies, "dap", split_axis=0, concat_axis=0, tiled=True)
    proj, scores = call(
        functools.partial(row_scores_body, head_size=head_size),
        [
            ((sequences, residues, 5 * channels), BF16, True),
            ((sequences, groups, residues, LANES // head_size * residues), F32, True),
        ],
        [homolog_features, horizontal_attend_entry_maps],
        flops=10**9,
    )
    [sent] = call(
        functools.partial(row_body, blocks=width, heads=heads, head_size=head_size),
        [((sequences * residues * tiles, LANES), BF16, True)],
        [bias, proj, scores, horizontal_attend_exit_map],
        scratch=[
            pltpu.VMEM((width * heads * rows, residues), F32),
            pltpu.VMEM((heads, residues, residues), F32),
            pltpu.VMEM((sequences * residues * tiles, LANES), F32),
        ],
    )
    received = lax.all_to_all(sent, "dap", split_axis=0, concat_axis=0, tiled=True)
    alignment, left, right = call(
        functools.partial(column_body, rows=rows, head_size=head_size),
        [
            ((count * rows * tiles, LANES), BF16, False),
            ((lanes, count), BF16, True),
            ((rows * span, count), BF16, True),
        ],
        [received, vertical_attend_entry_maps, vertical_attend_exit_map, tensor_product_factors.T],
        scratch=[pltpu.VMEM((count * rows * tiles, LANES), F32)] * 2,
    )
    pieces, order = gather_blocks(right)
    exit_map, left = lax.optimization_barrier((tensor_product_exit_map, left))
    [table] = call(
        functools.partial(table_body, rows=rows, lanes=lanes),
        [((span * lanes, 2 * depth), BF16, True)],
        [exit_map],
        scratch=[pltpu.VMEM((span * span, depth), F32)],
        flops=10**9,
    )
    [pair_output] = call(
        functools.partial(outer_body, order=tuple(order), span=span, count=count),
        [(twofold_features.shape, BF16, False)],
        [
            lax.axis_index("dap").astype(jnp.int32).reshape(1),
            left,
            *pieces,
            twofold_features,
            table,
        ],
        scratch=[
            pltpu.VMEM((span * residues, lanes), F32),
            pltpu.VMEM((rows // 2 * residues, span * lanes), BF16),
        ],
    )
    alignment = alignment.reshape(count, tiles, rows, LANES).transpose(0, 2, 1, 3)
    return (alignment.reshape(count, rows, channels), pair_output)


def solution(mesh):
    in_specs = (
        P(("crop", "dap"), None, None),
        P(("crop", "dap"), None, None),
        P(),
        P(),
        P(),
        P(),
        P(),
        P(),
        P(),
    )
    out_specs = (P("crop", "dap", None), P(("crop", "dap"), None, None))
    return jax.shard_map(
        per_device, mesh=mesh, in_specs=in_specs, out_specs=out_specs, check_vma=False
    )
```

```python
import functools
import math

import jax
import jax.numpy as jnp
from jax import lax
from jax.experimental import pallas as pl
from jax.experimental.pallas import tpu as pltpu
from jax.sharding import PartitionSpec as P

EPSILON = 1e-05
LANES = 128
F32 = jnp.float32
BF16 = jnp.bfloat16
VMEM = pl.BlockSpec(memory_space=pltpu.VMEM)
SMEM = pl.BlockSpec(memory_space=pltpu.SMEM)


def standardize(values):
    center = values - jnp.mean(values, axis=-1, keepdims=True)
    spread = jnp.mean(center * center, axis=-1, keepdims=True)
    return (center * lax.rsqrt(spread + EPSILON)).astype(BF16)


def dot(left, right):
    return jnp.dot(left, right, preferred_element_type=F32)


def dot_t(left, right):
    return lax.dot_general(left, right, (((1,), (1,)), ((), ())), preferred_element_type=F32)


def call(body, out_shapes, args, scratch=(), limit=16 << 20, flops=0, far=()):
    scalars = [jnp.issubdtype(arg.dtype, jnp.integer) for arg in args]
    return pl.pallas_call(
        body,
        out_shape=[
            pltpu.VMEM(shape, dtype) if near else jax.ShapeDtypeStruct(shape, dtype)
            for shape, dtype, near in out_shapes
        ],
        in_specs=[SMEM if scalar else VMEM for scalar in scalars],
        out_specs=[VMEM] * len(out_shapes),
        scratch_shapes=list(scratch),
        cost_estimate=pl.CostEstimate(flops=flops, bytes_accessed=0, transcendentals=0),
        compiler_params=pltpu.CompilerParams(vmem_limit_bytes=limit),
    )(*[
        arg
        if scalar
        else pltpu.with_memory_space_constraint(arg, pltpu.HBM if at in far else pltpu.VMEM)
        for at, (arg, scalar) in enumerate(zip(args, scalars))
    ])


def lane_masks(width, rows):
    lane = lax.broadcasted_iota(jnp.int32, (rows, LANES), 1)
    return [
        (lane >= start) & (lane < start + width) for start in range(0, LANES, width)
    ]


def masked_rows(block, masks):
    zero = jnp.zeros_like(block)
    return jnp.concatenate([jnp.where(mask, block, zero) for mask in masks], axis=0)


def bias_body(pair_ref, map_ref, out_ref):
    rows, _, _ = pair_ref.shape
    heads = map_ref.shape[0]
    height = heads * rows
    row = lax.broadcasted_iota(jnp.int32, (height, heads), 0)
    head = lax.broadcasted_iota(jnp.int32, (height, heads), 1)
    total = None
    for at in range(rows):
        spread = jnp.where(row == head * rows + at, 1.0, 0.0).astype(BF16)
        weights = dot(spread, map_ref[...]).astype(BF16)
        part = dot_t(weights, standardize(pair_ref[at].astype(F32)))
        total = part if total is None else total + part
    out_ref[...] = total.astype(BF16)


def scores_of(proj, head_size, masks):
    width = proj.shape[1] // 4
    scale = 1.0 / math.sqrt(head_size)
    scores = []
    for start in range(0, width, LANES):
        queries = proj[:, start : start + LANES]
        keys = masked_rows(proj[:, width + start : width + start + LANES], masks)
        scores.append(dot_t(queries, keys) * scale)
    return scores


def attended_of(scores, values, gates, masks):
    keys = values.shape[0]
    pieces = []
    for at in range(len(masks)):
        piece = scores[at]
        highest = jnp.max(piece, axis=-1, keepdims=True)
        pieces.append(jnp.exp(piece - highest).astype(BF16))
    ones = jnp.ones((keys, LANES), BF16)
    table = jnp.concatenate([masked_rows(values, masks), masked_rows(ones, masks)], axis=1)
    sums = dot(jnp.concatenate(pieces, axis=1), table)
    gate = jax.nn.sigmoid(gates.astype(F32))
    return (gate * (sums[:, :LANES] / sums[:, LANES:])).astype(BF16)


def row_scores_body(features_ref, maps_ref, exit_ref, proj_ref, scores_ref, kept_ref, *, head_size):
    sequences, residues, channels = features_ref.shape
    features = features_ref[...].reshape(sequences * residues, channels)
    proj_ref[:, 4 * channels :] = features
    kept_ref[...] = exit_ref[...]
    proj_ref[:, : 4 * channels] = dot(standardize(features.astype(F32)), maps_ref[...]).astype(BF16)
    masks = lane_masks(head_size, residues)
    for at in range(sequences):
        proj = proj_ref[at * residues : (at + 1) * residues, : 4 * channels]
        for block, scores in enumerate(scores_of(proj, head_size, masks)):
            scores_ref[at, block] = scores


def row_body(me_ref, *refs, order, heads, head_size, sequences):
    bias_refs = refs[:-7]
    proj_ref, scores_ref, exit_ref, out_ref, wide, bias, sent = refs[-7:]
    residues = proj_ref.shape[0] // sequences
    channels = exit_ref.shape[0]
    tiles = channels // LANES
    blocks = len(order)
    rows = residues // blocks
    at = 0
    for bias_ref in bias_refs:
        for block in range(bias_ref.shape[0] // (heads * rows)):
            source = jnp.bitwise_xor(me_ref[0], order[at])
            start = pl.multiple_of(source * (heads * rows), heads * rows)
            wide[pl.ds(start, heads * rows), :] = bias_ref[
                block * heads * rows : (block + 1) * heads * rows, :
            ].astype(F32)
            at += 1
    for source in range(blocks):
        for head in range(heads):
            start = (source * heads + head) * rows
            bias[head, source * rows : (source + 1) * rows, :] = wide[start : start + rows, :]
    masks = lane_masks(head_size, residues)
    for at in range(sequences):
        mine = slice(at * residues, (at + 1) * residues)
        gated = []
        for block, start in enumerate(range(0, channels, LANES)):
            scores = [
                scores_ref[at, block, :, k * residues : (k + 1) * residues]
                + bias[block * len(masks) + k]
                for k in range(len(masks))
            ]
            values = proj_ref[mine, 2 * channels + start : 2 * channels + start + LANES]
            gates = proj_ref[mine, 3 * channels + start : 3 * channels + start + LANES]
            gated.append(attended_of(scores, values, gates, masks))
        line = proj_ref[mine, 4 * channels :].astype(F32) + dot(
            jnp.concatenate(gated, axis=1), exit_ref[...]
        )
        for target in range(blocks):
            for tile in range(tiles):
                start = ((target * sequences + at) * tiles + tile) * rows
                sent[start : start + rows, :] = line[
                    target * rows : (target + 1) * rows, tile * LANES : (tile + 1) * LANES
                ]
    out_ref[...] = sent[...].astype(BF16)


def column_body(
    received_ref, maps_ref, exit_ref, factors_ref, out_ref, left_ref, right_ref, wide, done, proj_ref, score_ref,
    *, rows, head_size
):
    channels = maps_ref.shape[0]
    tiles = channels // LANES
    sequences = received_ref.shape[0] // (rows * tiles)
    span = factors_ref.shape[0] // 2
    wide[...] = received_ref[...].astype(F32)
    if left_ref.shape[0] > rows * span:
        left_ref[...] = jnp.zeros_like(left_ref)
    masks = lane_masks(head_size, sequences)
    chosen = [
        [pl.ds(tile * rows + at, sequences, stride=tiles * rows) for tile in range(tiles)]
        for at in range(rows)
    ]
    lines = jnp.concatenate(
        [jnp.concatenate([wide[rows_of, :] for rows_of in one], axis=1) for one in chosen], axis=0
    )
    proj_ref[...] = dot(standardize(lines), maps_ref[...]).astype(BF16)
    for at in range(rows):
        proj = proj_ref[at * sequences : (at + 1) * sequences, :]
        for block, scores in enumerate(scores_of(proj, head_size, masks)):
            score_ref[at, block] = scores
    gated = []
    for at in range(rows):
        mine = slice(at * sequences, (at + 1) * sequences)
        parts = []
        for block, start in enumerate(range(0, channels, LANES)):
            scores = [
                score_ref[at, block, :, k * sequences : (k + 1) * sequences] for k in range(len(masks))
            ]
            values = proj_ref[mine, 2 * channels + start : 2 * channels + start + LANES]
            gates = proj_ref[mine, 3 * channels + start : 3 * channels + start + LANES]
            parts.append(attended_of(scores, values, gates, masks))
        gated.append(jnp.concatenate(parts, axis=1))
    lines = lines + dot(jnp.concatenate(gated, axis=0), exit_ref[...])
    lines = lines.astype(BF16).astype(F32)
    factors = dot_t(factors_ref[...], standardize(lines)).astype(BF16)
    for at in range(rows):
        mine = slice(at * sequences, (at + 1) * sequences)
        left_ref[at * span : (at + 1) * span, :] = factors[:span, mine]
        right_ref[at * span : (at + 1) * span, :] = factors[span:, mine]
        for tile, rows_of in enumerate(chosen[at]):
            done[rows_of, :] = lines[mine, tile * LANES : (tile + 1) * LANES]
    out_ref[...] = done[...].astype(BF16)


def copy_body(from_ref, to_ref):
    to_ref[...] = from_ref[...]


def table_body(exit_ref, out_ref, wide, *, rows, lanes):
    depth = exit_ref.shape[1]
    span = out_ref.shape[0] // lanes
    wide[...] = exit_ref[...].astype(F32)
    zero = jnp.zeros((span, depth), BF16)
    for e in range(span):
        weights = wide[pl.ds(e, span, stride=span), :].astype(BF16)
        for row in range(rows):
            start = e * lanes + row * span
            side = [weights, zero] if row % 2 == 0 else [zero, weights]
            out_ref[start : start + span, :] = jnp.concatenate(side, axis=1)
        if lanes > rows * span:
            start = e * lanes + rows * span
            out_ref[start : (e + 1) * lanes, :] = jnp.zeros((lanes - rows * span, 2 * depth), BF16)


def outer_body(me_ref, left_ref, *refs, order, span, count):
    right_refs = refs[:-5]
    pair_ref, table_ref, out_ref, product, lhs = refs[-5:]
    rows, residues, depth = pair_ref.shape
    width = rows * span
    lanes = left_ref.shape[0]
    scale = 1.0 / count
    at = 0
    for right_ref in right_refs:
        for block in range(right_ref.shape[0] // width):
            source = jnp.bitwise_xor(me_ref[0], order[at])
            start = pl.multiple_of(source * width, width)
            product[pl.ds(start, width), :] = (
                dot_t(right_ref[block * width : (block + 1) * width, :], left_ref[...]) * scale
            )
            at += 1
    pairs = rows // 2
    lane = lax.broadcasted_iota(jnp.int32, (residues, lanes), 1)
    for e in range(span):
        part = product[pl.ds(e, residues, stride=span), :]
        for pair in range(pairs):
            start = pair * 2 * span
            keep = part if pairs == 1 else jnp.where((lane >= start) & (lane < start + 2 * span), part, 0.0)
            lhs[pair * residues : (pair + 1) * residues, e * lanes : (e + 1) * lanes] = keep.astype(BF16)
    delta = dot(lhs[...], table_ref[...])
    for row in range(rows):
        start = (row // 2) * residues
        out_ref[row] = (
            pair_ref[row].astype(F32)
            + delta[start : start + residues, (row % 2) * depth : (row % 2 + 1) * depth]
        ).astype(BF16)


def gather_rounds(width):
    rounds = []
    stride = width
    while stride > 1:
        radix = 4 if stride % 4 == 0 else 2
        stride //= radix
        rounds.append([step * stride for step in reversed(range(1, radix))])
    return rounds


def gather_blocks(block, beside=()):
    width = lax.axis_size("dap")
    pieces = [block]
    order = [0]
    for at, steps in enumerate(gather_rounds(width)):
        stacked = jnp.concatenate(pieces, axis=0) if len(pieces) > 1 else pieces[0]
        if 0 < at <= len(beside):
            stacked, _ = lax.optimization_barrier((stacked, beside[at - 1]))
        pieces = [stacked] + [
            lax.ppermute(stacked, "dap", [(d, d ^ step) for d in range(width)])
            for step in steps
        ]
        order = order + [k ^ step for step in steps for k in order]
    return pieces, order


def per_device(
    homolog_features,
    twofold_features,
    twofold_offset_map,
    horizontal_attend_entry_maps,
    horizontal_attend_exit_map,
    vertical_attend_entry_maps,
    vertical_attend_exit_map,
    tensor_product_factors,
    tensor_product_exit_map,
):
    width = lax.axis_size("dap")
    sequences, residues, channels = homolog_features.shape
    rows, _, depth = twofold_features.shape
    heads = twofold_offset_map.shape[1]
    head_size = channels // heads
    groups = channels // LANES
    span = tensor_product_factors.shape[1] // 2
    count = sequences * width
    lanes = max(rows * span, LANES)
    tiles = channels // LANES

    me = lax.axis_index("dap").astype(jnp.int32).reshape(1)

    [bias] = call(
        bias_body,
        [((heads * rows, residues), BF16, True)],
        [twofold_features, twofold_offset_map.T],
        far=(0, 1),
    )
    proj, scores, row_exit = call(
        functools.partial(row_scores_body, head_size=head_size),
        [
            ((sequences * residues, 5 * channels), BF16, True),
            ((sequences, groups, residues, LANES // head_size * residues), F32, True),
            (horizontal_attend_exit_map.shape, BF16, True),
        ],
        [homolog_features, horizontal_attend_entry_maps, horizontal_attend_exit_map],
        far=(0, 1, 2),
        flops=10**9,
    )
    bias_pieces, order = gather_blocks(bias, (proj,))
    [sent] = call(
        functools.partial(row_body, order=tuple(order), heads=heads, head_size=head_size, sequences=sequences),
        [((sequences * residues * tiles, LANES), BF16, True)],
        [me, *bias_pieces, proj, scores, row_exit],
        scratch=[
            pltpu.VMEM((width * heads * rows, residues), F32),
            pltpu.VMEM((heads, residues, residues), F32),
            pltpu.VMEM((sequences * residues * tiles, LANES), F32),
        ],
    )
    received = lax.all_to_all(sent, "dap", split_axis=0, concat_axis=0, tiled=True)
    alignment, left, right = call(
        functools.partial(column_body, rows=rows, head_size=head_size),
        [
            ((count * rows * tiles, LANES), BF16, True),
            ((lanes, count), BF16, True),
            ((rows * span, count), BF16, True),
        ],
        [received, vertical_attend_entry_maps, vertical_attend_exit_map, tensor_product_factors.T],
        scratch=[
            pltpu.VMEM((count * rows * tiles, LANES), F32),
            pltpu.VMEM((count * rows * tiles, LANES), F32),
            pltpu.VMEM((count * rows, 4 * channels), BF16),
            pltpu.VMEM((rows, groups, count, LANES // head_size * count), F32),
        ],
    )
    [table] = call(
        functools.partial(table_body, rows=rows, lanes=lanes),
        [((span * lanes, 2 * depth), BF16, True)],
        [lax.optimization_barrier((tensor_product_exit_map, left))[0]],
        scratch=[pltpu.VMEM((span * span, depth), F32)],
        flops=10**9,
    )
    [alignment] = call(copy_body, [(alignment.shape, BF16, False)], [alignment], flops=10**9)
    pieces, order = gather_blocks(right, (table, alignment))
    [pair_output] = call(
        functools.partial(outer_body, order=tuple(order), span=span, count=count),
        [(twofold_features.shape, BF16, False)],
        [
            me,
            left,
            *pieces,
            twofold_features,
            table,
        ],
        scratch=[
            pltpu.VMEM((span * residues, lanes), F32),
            pltpu.VMEM((rows // 2 * residues, span * lanes), BF16),
        ],
    )
    alignment = alignment.reshape(count, tiles, rows, LANES).transpose(0, 2, 1, 3)
    return (alignment.reshape(count, rows, channels), pair_output)


def solution(mesh):
    in_specs = (
        P(("crop", "dap"), None, None),
        P(("crop", "dap"), None, None),
        P(),
        P(),
        P(),
        P(),
        P(),
        P(),
        P(),
    )
    out_specs = (P("crop", "dap", None), P(("crop", "dap"), None, None))
    return jax.shard_map(
        per_device, mesh=mesh, in_specs=in_specs, out_specs=out_specs, check_vma=False
    )
```

```python
import functools
import math

import jax
import jax.numpy as jnp
from jax import lax
from jax.experimental import pallas as pl
from jax.experimental.pallas import tpu as pltpu
from jax.sharding import PartitionSpec as P

EPSILON = 1e-05
LANES = 128
F32 = jnp.float32
BF16 = jnp.bfloat16
VMEM = pl.BlockSpec(memory_space=pltpu.VMEM)
SMEM = pl.BlockSpec(memory_space=pltpu.SMEM)


def standardize(values):
    center = values - jnp.mean(values, axis=-1, keepdims=True)
    spread = jnp.mean(center * center, axis=-1, keepdims=True)
    return (center * lax.rsqrt(spread + EPSILON)).astype(BF16)


def dot(left, right):
    return jnp.dot(left, right, preferred_element_type=F32)


def dot_t(left, right):
    return lax.dot_general(left, right, (((1,), (1,)), ((), ())), preferred_element_type=F32)


def call(body, out_shapes, args, scratch=(), limit=16 << 20, flops=0, far=()):
    scalars = [jnp.issubdtype(arg.dtype, jnp.integer) for arg in args]
    return pl.pallas_call(
        body,
        out_shape=[
            pltpu.VMEM(shape, dtype) if near else jax.ShapeDtypeStruct(shape, dtype)
            for shape, dtype, near in out_shapes
        ],
        in_specs=[SMEM if scalar else VMEM for scalar in scalars],
        out_specs=[VMEM] * len(out_shapes),
        scratch_shapes=list(scratch),
        cost_estimate=pl.CostEstimate(flops=flops, bytes_accessed=0, transcendentals=0),
        compiler_params=pltpu.CompilerParams(vmem_limit_bytes=limit),
    )(*[
        arg
        if scalar
        else pltpu.with_memory_space_constraint(arg, pltpu.HBM if at in far else pltpu.VMEM)
        for at, (arg, scalar) in enumerate(zip(args, scalars))
    ])


def lane_masks(width, rows):
    lane = lax.broadcasted_iota(jnp.int32, (rows, LANES), 1)
    return [
        (lane >= start) & (lane < start + width) for start in range(0, LANES, width)
    ]


def masked_rows(block, masks):
    zero = jnp.zeros_like(block)
    return jnp.concatenate([jnp.where(mask, block, zero) for mask in masks], axis=0)


def bias_body(pair_ref, map_ref, out_ref, *, copies):
    rows, _, _ = pair_ref.shape
    heads = map_ref.shape[0]
    height = heads * rows
    row = lax.broadcasted_iota(jnp.int32, (height, heads), 0)
    head = lax.broadcasted_iota(jnp.int32, (height, heads), 1)
    total = None
    for at in range(rows):
        spread = jnp.where(row == head * rows + at, 1.0, 0.0).astype(BF16)
        weights = dot(spread, map_ref[...]).astype(BF16)
        part = dot_t(weights, standardize(pair_ref[at].astype(F32)))
        total = part if total is None else total + part
    block = total.astype(BF16)
    half = height // 2
    for copy in range(copies):
        out_ref[copy * half : (copy + 1) * half, :] = block[copy % 2 * half : (copy % 2 + 1) * half, :]


def scores_of(proj, head_size, masks):
    width = proj.shape[1] // 4
    scale = 1.0 / math.sqrt(head_size)
    scores = []
    for start in range(0, width, LANES):
        queries = proj[:, start : start + LANES]
        keys = masked_rows(proj[:, width + start : width + start + LANES], masks)
        scores.append(dot_t(queries, keys) * scale)
    return scores


def attended_of(scores, values, gates, masks):
    keys = values.shape[0]
    pieces = []
    for at in range(len(masks)):
        piece = scores[at]
        highest = jnp.max(piece, axis=-1, keepdims=True)
        pieces.append(jnp.exp(piece - highest).astype(BF16))
    ones = jnp.ones((keys, LANES), BF16)
    table = jnp.concatenate([masked_rows(values, masks), masked_rows(ones, masks)], axis=1)
    sums = dot(jnp.concatenate(pieces, axis=1), table)
    gate = jax.nn.sigmoid(gates.astype(F32))
    return (gate * (sums[:, :LANES] / sums[:, LANES:])).astype(BF16)


def row_scores_body(features_ref, maps_ref, kept_ref, scores_ref, *, head_size):
    sequences, residues, channels = features_ref.shape
    features = features_ref[...].reshape(sequences * residues, channels)
    proj = dot(standardize(features.astype(F32)), maps_ref[...]).astype(BF16)
    for block, start in enumerate(range(0, channels, LANES)):
        kept_ref[block, :, :LANES] = proj[:, 2 * channels + start : 2 * channels + start + LANES]
        kept_ref[block, :, LANES : 2 * LANES] = proj[:, 3 * channels + start : 3 * channels + start + LANES]
        kept_ref[block, :, 2 * LANES :] = features[:, start : start + LANES]
    masks = lane_masks(head_size, residues)
    for at in range(sequences):
        mine = proj[at * residues : (at + 1) * residues, :]
        for block, scores in enumerate(scores_of(mine, head_size, masks)):
            scores_ref[at, block] = scores


def row_half(bias_ref, kept_ref, scores_ref, wide, bias, first, blocks, head_size):
    sequences, _, residues, _ = scores_ref.shape
    rows = residues // blocks
    heads = bias_ref.shape[0] // residues
    masks = lane_masks(head_size, residues)
    wide[...] = bias_ref[...].astype(F32)
    for source in range(blocks):
        for head in range(heads):
            start = (source * heads + head) * rows
            bias[head, source * rows : (source + 1) * rows, :] = wide[start : start + rows, :]
    gated = []
    for block in range(heads // len(masks)):
        parts = []
        for at in range(sequences):
            mine = pl.ds(at * residues, residues)
            scores = [
                scores_ref[at, first + block, :, k * residues : (k + 1) * residues]
                + bias[block * len(masks) + k]
                for k in range(len(masks))
            ]
            values = kept_ref[first + block, mine, :LANES]
            gates = kept_ref[first + block, mine, LANES : 2 * LANES]
            parts.append(attended_of(scores, values, gates, masks))
        gated.append(parts)
    return gated


def row_first_body(me_ref, bias_ref, kept_ref, scores_ref, out_ref, wide, bias, *, blocks, head_size):
    groups = kept_ref.shape[0] // 2
    residues = scores_ref.shape[2]
    first = jnp.bitwise_and(me_ref[0], 1) * groups
    gated = row_half(bias_ref, kept_ref, scores_ref, wide, bias, first, blocks, head_size)
    for block, parts in enumerate(gated):
        for at, part in enumerate(parts):
            out_ref[block, at * residues : (at + 1) * residues, :] = part


def row_second_body(
    me_ref, bias_ref, kept_ref, scores_ref, gated_ref, exit_ref, out_ref, wide, bias, sent, *, blocks, head_size
):
    groups = kept_ref.shape[0] // 2
    sequences, tiles, residues, _ = scores_ref.shape
    rows = residues // blocks
    parity = jnp.bitwise_and(me_ref[0], 1)
    gated = row_half(bias_ref, kept_ref, scores_ref, wide, bias, (1 - parity) * groups, blocks, head_size)

    def exit_rows(group):
        return exit_ref[pl.ds(pl.multiple_of(group * LANES, LANES), LANES), :]

    for at in range(sequences):
        mine = slice(at * residues, (at + 1) * residues)
        delta = None
        for block in range(groups):
            for part, group in (
                (gated_ref[block, mine, :], parity * groups + block),
                (gated[block][at], (1 - parity) * groups + block),
            ):
                more = dot(part, exit_rows(group))
                delta = more if delta is None else delta + more
        for tile in range(tiles):
            line = kept_ref[tile, mine, 2 * LANES :].astype(F32) + delta[:, tile * LANES : (tile + 1) * LANES]
            for target in range(blocks):
                start = ((target * sequences + at) * tiles + tile) * rows
                sent[start : start + rows, :] = line[target * rows : (target + 1) * rows, :]
    out_ref[...] = sent[...].astype(BF16)


def column_body(
    received_ref, maps_ref, exit_ref, factors_ref, out_ref, left_ref, right_ref, wide, done, proj_ref, score_ref,
    *, rows, head_size
):
    channels = maps_ref.shape[0]
    tiles = channels // LANES
    sequences = received_ref.shape[0] // (rows * tiles)
    span = factors_ref.shape[0] // 2
    wide[...] = received_ref[...].astype(F32)
    if left_ref.shape[0] > rows * span:
        left_ref[...] = jnp.zeros_like(left_ref)
    masks = lane_masks(head_size, sequences)
    chosen = [
        [pl.ds(tile * rows + at, sequences, stride=tiles * rows) for tile in range(tiles)]
        for at in range(rows)
    ]
    lines = jnp.concatenate(
        [jnp.concatenate([wide[rows_of, :] for rows_of in one], axis=1) for one in chosen], axis=0
    )
    proj_ref[...] = dot(standardize(lines), maps_ref[...]).astype(BF16)
    for at in range(rows):
        proj = proj_ref[at * sequences : (at + 1) * sequences, :]
        for block, scores in enumerate(scores_of(proj, head_size, masks)):
            score_ref[at, block] = scores
    gated = []
    for at in range(rows):
        mine = slice(at * sequences, (at + 1) * sequences)
        parts = []
        for block, start in enumerate(range(0, channels, LANES)):
            scores = [
                score_ref[at, block, :, k * sequences : (k + 1) * sequences] for k in range(len(masks))
            ]
            values = proj_ref[mine, 2 * channels + start : 2 * channels + start + LANES]
            gates = proj_ref[mine, 3 * channels + start : 3 * channels + start + LANES]
            parts.append(attended_of(scores, values, gates, masks))
        gated.append(jnp.concatenate(parts, axis=1))
    lines = lines + dot(jnp.concatenate(gated, axis=0), exit_ref[...])
    lines = lines.astype(BF16).astype(F32)
    factors = dot_t(factors_ref[...], standardize(lines)).astype(BF16)
    for at in range(rows):
        mine = slice(at * sequences, (at + 1) * sequences)
        left_ref[at * span : (at + 1) * span, :] = factors[:span, mine]
        right_ref[at * span : (at + 1) * span, :] = factors[span:, mine]
        for tile, rows_of in enumerate(chosen[at]):
            done[rows_of, :] = lines[mine, tile * LANES : (tile + 1) * LANES]
    out_ref[...] = done[...].astype(BF16)


def copy_body(from_ref, to_ref):
    to_ref[...] = from_ref[...]


def table_body(exit_ref, out_ref, wide, *, rows, lanes):
    depth = exit_ref.shape[1]
    span = out_ref.shape[0] // lanes
    wide[...] = exit_ref[...].astype(F32)
    zero = jnp.zeros((span, depth), BF16)
    for e in range(span):
        weights = wide[pl.ds(e, span, stride=span), :].astype(BF16)
        for row in range(rows):
            start = e * lanes + row * span
            side = [weights, zero] if row % 2 == 0 else [zero, weights]
            out_ref[start : start + span, :] = jnp.concatenate(side, axis=1)
        if lanes > rows * span:
            start = e * lanes + rows * span
            out_ref[start : (e + 1) * lanes, :] = jnp.zeros((lanes - rows * span, 2 * depth), BF16)


def outer_delta(me_ref, left_ref, right_ref, table_ref, product, lhs, order, radix, span, count, rows):
    width = rows * span
    lanes = left_ref.shape[0]
    residues = product.shape[0] // span
    mine = me_ref[0] // radix
    for at, step in enumerate(order):
        source = jnp.bitwise_xor(mine, step // radix)
        start = pl.multiple_of(source * width, width)
        product[pl.ds(start, width), :] = (
            dot_t(right_ref[at * width : (at + 1) * width, :], left_ref[...]) * (1.0 / count)
        )
    pairs = rows // 2
    lane = lax.broadcasted_iota(jnp.int32, (residues, lanes), 1)
    for e in range(span):
        part = product[pl.ds(e, residues, stride=span), :]
        for pair in range(pairs):
            start = pair * 2 * span
            keep = part if pairs == 1 else jnp.where((lane >= start) & (lane < start + 2 * span), part, 0.0)
            lhs[pair * residues : (pair + 1) * residues, e * lanes : (e + 1) * lanes] = keep.astype(BF16)
    return dot(lhs[...], table_ref[...])


def outer_first_body(me_ref, left_ref, right_ref, table_ref, out_ref, product, lhs, **sizes):
    out_ref[...] = outer_delta(me_ref, left_ref, right_ref, table_ref, product, lhs, **sizes)


def outer_last_body(me_ref, left_ref, *refs, radix, rows, **sizes):
    right_refs = refs[: radix - 1]
    table_ref, first_ref, pair_ref, out_ref, product, lhs, chosen, stage = refs[radix - 1 :]
    depth = pair_ref.shape[2]
    deltas = [first_ref[...]] + [
        outer_delta(me_ref, left_ref, right_ref, table_ref, product, lhs, radix=radix, rows=rows, **sizes)
        for right_ref in right_refs
    ]
    digit = me_ref[0] % radix
    for place in range(radix):
        value = deltas[0]
        for piece in range(1, radix):
            value = jnp.where(jnp.bitwise_xor(digit, piece) == place, deltas[piece], value)
        chosen[place] = value
    residues = chosen.shape[1] // (rows // 2)
    for row in range(rows):
        side = slice((row % 2) * depth, (row % 2 + 1) * depth)
        for source in range(residues // rows):
            for place in range(radix):
                start = (row // 2) * residues + source * rows
                to = (source * radix + place) * rows
                stage[row, to : to + rows, :] = chosen[place, start : start + rows, side]
        out_ref[row] = (pair_ref[row].astype(F32) + stage[row]).astype(BF16)


def gather_rounds(width):
    rounds = []
    stride = width
    while stride > 1:
        radix = 4 if stride % 4 == 0 else 2
        stride //= radix
        rounds.append([step * stride for step in reversed(range(1, radix))])
    return rounds


def gather_blocks(block, beside=()):
    width = lax.axis_size("dap")
    pieces = [block]
    order = [0]
    for at, steps in enumerate(gather_rounds(width)):
        stacked = jnp.concatenate(pieces, axis=0) if len(pieces) > 1 else pieces[0]
        if 0 < at <= len(beside):
            stacked, _ = lax.optimization_barrier((stacked, beside[at - 1]))
        pieces = [stacked] + [
            lax.ppermute(stacked, "dap", [(d, d ^ step) for d in range(width)])
            for step in steps
        ]
        order = order + [k ^ step for step in steps for k in order]
    return pieces, order


def per_device(
    homolog_features,
    twofold_features,
    twofold_offset_map,
    horizontal_attend_entry_maps,
    horizontal_attend_exit_map,
    vertical_attend_entry_maps,
    vertical_attend_exit_map,
    tensor_product_factors,
    tensor_product_exit_map,
):
    width = lax.axis_size("dap")
    sequences, residues, channels = homolog_features.shape
    rows, _, depth = twofold_features.shape
    heads = twofold_offset_map.shape[1]
    head_size = channels // heads
    groups = channels // LANES
    span = tensor_product_factors.shape[1] // 2
    count = sequences * width
    lanes = max(rows * span, LANES)
    tiles = channels // LANES

    me = lax.axis_index("dap").astype(jnp.int32).reshape(1)

    [halves] = call(
        functools.partial(bias_body, copies=width),
        [((width * heads * rows // 2, residues), BF16, False)],
        [twofold_features, twofold_offset_map.T],
        far=(0, 1),
    )
    features, halves = lax.optimization_barrier((homolog_features, halves))
    own = lax.all_to_all(halves, "dap", split_axis=0, concat_axis=0, tiled=True)
    kept, scores = call(
        functools.partial(row_scores_body, head_size=head_size),
        [
            ((groups, sequences * residues, 3 * LANES), BF16, True),
            ((sequences, groups, residues, LANES // head_size * residues), F32, True),
        ],
        [features, horizontal_attend_entry_maps],
        far=(0, 1),
        flops=10**9,
    )
    own, scores = lax.optimization_barrier((own, scores))
    other = lax.ppermute(own, "dap", [(d, d ^ 1) for d in range(width)])
    bias_scratch = [
        pltpu.VMEM((width * heads * rows // 2, residues), F32),
        pltpu.VMEM((heads // 2, residues, residues), F32),
    ]
    [gated] = call(
        functools.partial(row_first_body, blocks=width, head_size=head_size),
        [((groups // 2, sequences * residues, LANES), BF16, True)],
        [me, own, kept, scores],
        scratch=bias_scratch,
        flops=10**9,
    )
    [sent] = call(
        functools.partial(row_second_body, blocks=width, head_size=head_size),
        [((sequences * residues * tiles, LANES), BF16, True)],
        [me, other, kept, scores, gated, horizontal_attend_exit_map],
        scratch=bias_scratch + [pltpu.VMEM((sequences * residues * tiles, LANES), F32)],
    )
    received = lax.all_to_all(sent, "dap", split_axis=0, concat_axis=0, tiled=True)
    alignment, left, right = call(
        functools.partial(column_body, rows=rows, head_size=head_size),
        [
            ((count * rows * tiles, LANES), BF16, True),
            ((lanes, count), BF16, True),
            ((rows * span, count), BF16, True),
        ],
        [received, vertical_attend_entry_maps, vertical_attend_exit_map, tensor_product_factors.T],
        scratch=[
            pltpu.VMEM((count * rows * tiles, LANES), F32),
            pltpu.VMEM((count * rows * tiles, LANES), F32),
            pltpu.VMEM((count * rows, 4 * channels), BF16),
            pltpu.VMEM((rows, groups, count, LANES // head_size * count), F32),
        ],
    )
    [table] = call(
        functools.partial(table_body, rows=rows, lanes=lanes),
        [((span * lanes, 2 * depth), BF16, True)],
        [lax.optimization_barrier((tensor_product_exit_map, left))[0]],
        scratch=[pltpu.VMEM((span * span, depth), F32)],
        flops=10**9,
    )
    [alignment] = call(copy_body, [(alignment.shape, BF16, False)], [alignment], flops=10**9)
    pieces, order = gather_blocks(right, (table, alignment))
    radix = len(pieces)
    sizes = dict(order=tuple(order[: width // radix]), radix=radix, span=span, count=count, rows=rows)
    share = residues // radix
    scratch = [
        pltpu.VMEM((span * share, lanes), F32),
        pltpu.VMEM((rows // 2 * share, span * lanes), BF16),
    ]
    [first] = call(
        functools.partial(outer_first_body, **sizes),
        [((rows // 2 * share, 2 * depth), F32, True)],
        [me, left, pieces[0], table],
        scratch=scratch,
        flops=10**9,
    )
    [pair_output] = call(
        functools.partial(outer_last_body, **sizes),
        [(twofold_features.shape, BF16, False)],
        [me, left, *pieces[1:], table, first, twofold_features],
        scratch=scratch
        + [
            pltpu.VMEM((radix, rows // 2 * share, 2 * depth), F32),
            pltpu.VMEM((rows, residues, depth), F32),
        ],
    )
    alignment = alignment.reshape(count, tiles, rows, LANES).transpose(0, 2, 1, 3)
    return (alignment.reshape(count, rows, channels), pair_output)


def solution(mesh):
    in_specs = (
        P(("crop", "dap"), None, None),
        P(("crop", "dap"), None, None),
        P(),
        P(),
        P(),
        P(),
        P(),
        P(),
        P(),
    )
    out_specs = (P("crop", "dap", None), P(("crop", "dap"), None, None))
    return jax.shard_map(
        per_device, mesh=mesh, in_specs=in_specs, out_specs=out_specs, check_vma=False
    )
```

```python
import functools
import math

import jax
import jax.numpy as jnp
from jax import lax
from jax.experimental import pallas as pl
from jax.experimental.pallas import tpu as pltpu
from jax.sharding import PartitionSpec as P

EPSILON = 1e-05
LANES = 128
F32 = jnp.float32
BF16 = jnp.bfloat16
VMEM = pl.BlockSpec(memory_space=pltpu.VMEM)
SMEM = pl.BlockSpec(memory_space=pltpu.SMEM)


def standardize(values):
    center = values - jnp.mean(values, axis=-1, keepdims=True)
    spread = jnp.mean(center * center, axis=-1, keepdims=True)
    return (center * lax.rsqrt(spread + EPSILON)).astype(BF16)


def dot(left, right):
    return jnp.dot(left, right, preferred_element_type=F32)


def dot_t(left, right):
    return lax.dot_general(left, right, (((1,), (1,)), ((), ())), preferred_element_type=F32)


def call(body, out_shapes, args, scratch=(), limit=16 << 20, flops=0, far=()):
    scalars = [jnp.issubdtype(arg.dtype, jnp.integer) for arg in args]
    return pl.pallas_call(
        body,
        out_shape=[
            pltpu.VMEM(shape, dtype) if near else jax.ShapeDtypeStruct(shape, dtype)
            for shape, dtype, near in out_shapes
        ],
        in_specs=[SMEM if scalar else VMEM for scalar in scalars],
        out_specs=[VMEM] * len(out_shapes),
        scratch_shapes=list(scratch),
        cost_estimate=pl.CostEstimate(flops=flops, bytes_accessed=0, transcendentals=0),
        compiler_params=pltpu.CompilerParams(vmem_limit_bytes=limit),
    )(*[
        arg
        if scalar
        else pltpu.with_memory_space_constraint(arg, pltpu.HBM if at in far else pltpu.VMEM)
        for at, (arg, scalar) in enumerate(zip(args, scalars))
    ])


def lane_masks(width, rows):
    lane = lax.broadcasted_iota(jnp.int32, (rows, LANES), 1)
    return [
        (lane >= start) & (lane < start + width) for start in range(0, LANES, width)
    ]


def masked_rows(block, masks):
    zero = jnp.zeros_like(block)
    return jnp.concatenate([jnp.where(mask, block, zero) for mask in masks], axis=0)


def bias_body(pair_ref, map_ref, out_ref, *, copies):
    rows, _, _ = pair_ref.shape
    heads = map_ref.shape[0]
    height = heads * rows
    row = lax.broadcasted_iota(jnp.int32, (height, heads), 0)
    head = lax.broadcasted_iota(jnp.int32, (height, heads), 1)
    total = None
    for at in range(rows):
        spread = jnp.where(row == head * rows + at, 1.0, 0.0).astype(BF16)
        weights = dot(spread, map_ref[...]).astype(BF16)
        part = dot_t(weights, standardize(pair_ref[at].astype(F32)))
        total = part if total is None else total + part
    block = total.astype(BF16)
    half = height // 2
    for copy in range(copies):
        out_ref[copy * half : (copy + 1) * half, :] = block[copy % 2 * half : (copy % 2 + 1) * half, :]


def scores_of(proj, head_size, masks):
    width = proj.shape[1] // 4
    scale = 1.0 / math.sqrt(head_size)
    scores = []
    for start in range(0, width, LANES):
        queries = proj[:, start : start + LANES]
        keys = masked_rows(proj[:, width + start : width + start + LANES], masks)
        scores.append(dot_t(queries, keys) * scale)
    return scores


def attended_of(scores, values, gates, masks):
    keys = values.shape[0]
    pieces = []
    for at in range(len(masks)):
        piece = scores[at]
        highest = jnp.max(piece, axis=-1, keepdims=True)
        pieces.append(jnp.exp(piece - highest).astype(BF16))
    ones = jnp.ones((keys, LANES), BF16)
    table = jnp.concatenate([masked_rows(values, masks), masked_rows(ones, masks)], axis=1)
    sums = dot(jnp.concatenate(pieces, axis=1), table)
    gate = jax.nn.sigmoid(gates.astype(F32))
    return (gate * (sums[:, :LANES] / sums[:, LANES:])).astype(BF16)


def row_scores_body(features_ref, maps_ref, kept_ref, scores_ref, *, head_size):
    sequences, residues, channels = features_ref.shape
    features = features_ref[...].reshape(sequences * residues, channels)
    proj = dot(standardize(features.astype(F32)), maps_ref[...]).astype(BF16)
    for block, start in enumerate(range(0, channels, LANES)):
        kept_ref[block, :, :LANES] = proj[:, 2 * channels + start : 2 * channels + start + LANES]
        kept_ref[block, :, LANES : 2 * LANES] = proj[:, 3 * channels + start : 3 * channels + start + LANES]
        kept_ref[block, :, 2 * LANES :] = features[:, start : start + LANES]
    masks = lane_masks(head_size, residues)
    for at in range(sequences):
        mine = proj[at * residues : (at + 1) * residues, :]
        for block, scores in enumerate(scores_of(mine, head_size, masks)):
            scores_ref[at, block] = scores


def row_half(bias_ref, kept_ref, scores_ref, wide, bias, first, blocks, head_size):
    sequences, _, residues, _ = scores_ref.shape
    rows = residues // blocks
    heads = bias_ref.shape[0] // residues
    masks = lane_masks(head_size, residues)
    wide[...] = bias_ref[...].astype(F32)
    for source in range(blocks):
        for head in range(heads):
            start = (source * heads + head) * rows
            bias[head, source * rows : (source + 1) * rows, :] = wide[start : start + rows, :]
    gated = []
    for block in range(heads // len(masks)):
        parts = []
        for at in range(sequences):
            mine = pl.ds(at * residues, residues)
            scores = [
                scores_ref[at, first + block, :, k * residues : (k + 1) * residues]
                + bias[block * len(masks) + k]
                for k in range(len(masks))
            ]
            values = kept_ref[first + block, mine, :LANES]
            gates = kept_ref[first + block, mine, LANES : 2 * LANES]
            parts.append(attended_of(scores, values, gates, masks))
        gated.append(parts)
    return gated


def row_first_body(me_ref, bias_ref, kept_ref, scores_ref, out_ref, wide, bias, *, blocks, head_size):
    groups = kept_ref.shape[0] // 2
    residues = scores_ref.shape[2]
    first = jnp.bitwise_and(me_ref[0], 1) * groups
    gated = row_half(bias_ref, kept_ref, scores_ref, wide, bias, first, blocks, head_size)
    for block, parts in enumerate(gated):
        for at, part in enumerate(parts):
            out_ref[block, at * residues : (at + 1) * residues, :] = part


def row_second_body(
    me_ref, bias_ref, kept_ref, scores_ref, gated_ref, exit_ref, out_ref, wide, bias, sent, *, blocks, head_size
):
    groups = kept_ref.shape[0] // 2
    sequences, tiles, residues, _ = scores_ref.shape
    rows = residues // blocks
    parity = jnp.bitwise_and(me_ref[0], 1)
    gated = row_half(bias_ref, kept_ref, scores_ref, wide, bias, (1 - parity) * groups, blocks, head_size)

    def exit_rows(group):
        return exit_ref[pl.ds(pl.multiple_of(group * LANES, LANES), LANES), :]

    for at in range(sequences):
        mine = slice(at * residues, (at + 1) * residues)
        delta = None
        for block in range(groups):
            for part, group in (
                (gated_ref[block, mine, :], parity * groups + block),
                (gated[block][at], (1 - parity) * groups + block),
            ):
                more = dot(part, exit_rows(group))
                delta = more if delta is None else delta + more
        for tile in range(tiles):
            line = kept_ref[tile, mine, 2 * LANES :].astype(F32) + delta[:, tile * LANES : (tile + 1) * LANES]
            for target in range(blocks):
                start = ((target * sequences + at) * tiles + tile) * rows
                sent[start : start + rows, :] = line[target * rows : (target + 1) * rows, :]
    out_ref[...] = sent[...].astype(BF16)


def column_body(
    received_ref, maps_ref, exit_ref, factors_ref, lines_ref, left_ref, right_ref, wide, proj_ref, score_ref, turned,
    *, rows, head_size
):
    channels = maps_ref.shape[0]
    tiles = channels // LANES
    sequences = received_ref.shape[0] // (rows * tiles)
    span = factors_ref.shape[0] // 2
    wide[...] = received_ref[...].astype(F32)
    if left_ref.shape[0] > rows * span:
        left_ref[...] = jnp.zeros_like(left_ref)
    masks = lane_masks(head_size, sequences)
    chosen = [
        [pl.ds(tile * rows + at, sequences, stride=tiles * rows) for tile in range(tiles)]
        for at in range(rows)
    ]
    lines = jnp.concatenate(
        [jnp.concatenate([wide[rows_of, :] for rows_of in one], axis=1) for one in chosen], axis=0
    )
    proj_ref[...] = dot(standardize(lines), maps_ref[...]).astype(BF16)
    for at in range(rows):
        proj = proj_ref[at * sequences : (at + 1) * sequences, :]
        for block, scores in enumerate(scores_of(proj, head_size, masks)):
            score_ref[at, block] = scores
    gated = []
    for at in range(rows):
        mine = slice(at * sequences, (at + 1) * sequences)
        parts = []
        for block, start in enumerate(range(0, channels, LANES)):
            scores = [
                score_ref[at, block, :, k * sequences : (k + 1) * sequences] for k in range(len(masks))
            ]
            values = proj_ref[mine, 2 * channels + start : 2 * channels + start + LANES]
            gates = proj_ref[mine, 3 * channels + start : 3 * channels + start + LANES]
            parts.append(attended_of(scores, values, gates, masks))
        gated.append(jnp.concatenate(parts, axis=1))
    lines = lines + dot(jnp.concatenate(gated, axis=0), exit_ref[...])
    lines = lines.astype(BF16).astype(F32)
    lines_ref[...] = lines
    factors = dot_t(factors_ref[...], standardize(lines))
    for at in range(rows):
        mine = slice(at * sequences, (at + 1) * sequences)
        left_ref[at * span : (at + 1) * span, :] = factors[:span, mine].astype(BF16)
        turned[pl.ds(at, span, stride=rows), :] = factors[span:, mine]
    right_ref[...] = turned[...].astype(BF16)


def arrange_body(lines_ref, out_ref, done, *, rows):
    total, channels = lines_ref.shape
    sequences = total // rows
    tiles = channels // LANES
    for at in range(rows):
        for tile in range(tiles):
            done[pl.ds(tile * rows + at, sequences, stride=tiles * rows), :] = lines_ref[
                at * sequences : (at + 1) * sequences, tile * LANES : (tile + 1) * LANES
            ]
    out_ref[...] = done[...].astype(BF16)


def table_body(exit_ref, out_ref, wide):
    depth = exit_ref.shape[1]
    span = math.isqrt(exit_ref.shape[0])
    wide[...] = exit_ref[...].astype(F32)
    zero = jnp.zeros((span, depth), BF16)
    for e in range(span):
        weights = wide[pl.ds(e, span, stride=span), :].astype(BF16)
        for row, side in enumerate(([weights, zero], [zero, weights])):
            start = (2 * e + row) * span
            out_ref[start : start + span, :] = jnp.concatenate(side, axis=1)


def outer_rows(me_ref, left_ref, right_refs, out_ref, product, order, radix, span, count, rows):
    width = rows * span
    lanes = left_ref.shape[0]
    residues = len(order) * rows
    mine = me_ref[0] // radix
    left = left_ref[...]
    zero = jnp.zeros_like(left)
    both = jnp.concatenate(
        [jnp.concatenate([left, zero], axis=1), jnp.concatenate([zero, left], axis=1)], axis=0
    )
    half = len(order) // 2
    lane = lax.broadcasted_iota(jnp.int32, (residues, LANES), 1)
    for piece, right_ref in enumerate(right_refs):
        products = dot_t(
            jnp.concatenate([right_ref[: half * width, :], right_ref[half * width :, :]], axis=1), both
        ) * (1.0 / count)
        for at, step in enumerate(order):
            source = jnp.bitwise_xor(mine, step // radix)
            start = at % half * width
            side = at // half * lanes
            for tile in range(lanes // LANES):
                product[tile, source] = products[
                    start : start + width, side + tile * LANES : side + (tile + 1) * LANES
                ]
        for e in range(0, span, 2):
            for tile in range(lanes // LANES):
                halves = couple_of(product, tile, e, rows, residues)
                swapped = [pltpu.roll(part, LANES // 2, 1) for part in halves]
                for pair in range(2 * tile, min(2 * tile + 2, rows // 2)):
                    low, high = (halves[0], swapped[1]) if pair % 2 == 0 else (swapped[0], halves[1])
                    start = (piece * (rows // 2) + pair) * residues
                    out_ref[start : start + residues, e // 2 * LANES : (e // 2 + 1) * LANES] = jnp.where(
                        lane < LANES // 2, low, high
                    ).astype(BF16)


def couple_of(product, tile, e, rows, residues):
    if rows % 8 == 0:
        return [
            product[tile, :, (e + odd) * rows : (e + odd + 1) * rows, :].reshape(residues, LANES)
            for odd in (0, 1)
        ]
    couples = product[tile, :, e * rows : (e + 2) * rows, :]
    sources = couples.shape[0]
    if rows != 4:
        return [
            jnp.concatenate([couples[at, odd * rows : (odd + 1) * rows] for at in range(sources)], axis=0)
            for odd in (0, 1)
        ]
    couples = couples.reshape(sources // 2, 2, 2 * rows, LANES)
    first, second = couples[:, 0], couples[:, 1]
    upper = lax.broadcasted_iota(jnp.int32, first.shape, 1) < rows
    even = jnp.where(upper, first, pltpu.roll(second, rows, 1))
    odd = jnp.where(upper, pltpu.roll(first, rows, 1), second)
    return [part.reshape(residues, LANES) for part in (even, odd)]


def outer_first_body(me_ref, left_ref, right_ref, out_ref, product, **sizes):
    outer_rows(me_ref, left_ref, [right_ref], out_ref, product, **sizes)


def outer_last_body(me_ref, left_ref, *refs, radix, rows, **sizes):
    right_refs = refs[: radix - 1]
    table_ref, first_ref, pair_ref, out_ref, product, rest = refs[radix - 1 :]
    depth = pair_ref.shape[2]
    outer_rows(me_ref, left_ref, right_refs, rest, product, radix=radix, rows=rows, **sizes)
    delta = dot(jnp.concatenate([first_ref[...], rest[...]], axis=0), table_ref[...])
    height = first_ref.shape[0]
    residues = height // (rows // 2)
    digit = me_ref[0] % radix
    places = []
    for place in range(radix):
        value = delta[:height]
        for piece in range(1, radix):
            value = jnp.where(
                jnp.bitwise_xor(digit, piece) == place, delta[piece * height : (piece + 1) * height], value
            )
        places.append(value)
    for row in range(rows):
        block = slice((row // 2) * residues, (row // 2 + 1) * residues)
        side = slice((row % 2) * depth, (row % 2 + 1) * depth)
        more = interleave([value[block, side] for value in places], rows)
        out_ref[row] = (pair_ref[row].astype(F32) + more).astype(BF16)


def interleave(parts, rows):
    total, lanes = parts[0].shape
    if rows != 4 or len(parts) != 2:
        return jnp.concatenate(
            [part[at : at + rows] for at in range(0, total, rows) for part in parts], axis=0
        )
    first, second = [part.reshape(total // 8, 8, lanes) for part in parts]
    upper = lax.broadcasted_iota(jnp.int32, first.shape, 1) < rows
    even = jnp.where(upper, first, pltpu.roll(second, rows, 1))
    odd = jnp.where(upper, pltpu.roll(first, rows, 1), second)
    return jnp.concatenate([even[:, None], odd[:, None]], axis=1).reshape(2 * total, lanes)


def gather_rounds(width):
    rounds = []
    stride = width
    while stride > 1:
        radix = 4 if stride % 4 == 0 else 2
        stride //= radix
        rounds.append([step * stride for step in reversed(range(1, radix))])
    return rounds


def gather_blocks(block, beside=()):
    width = lax.axis_size("dap")
    pieces = [block]
    order = [0]
    for at, steps in enumerate(gather_rounds(width)):
        stacked = jnp.concatenate(pieces, axis=0) if len(pieces) > 1 else pieces[0]
        if 0 < at <= len(beside):
            stacked, _ = lax.optimization_barrier((stacked, beside[at - 1]))
        pieces = [stacked] + [
            lax.ppermute(stacked, "dap", [(d, d ^ step) for d in range(width)])
            for step in steps
        ]
        order = order + [k ^ step for step in steps for k in order]
    return pieces, order


def per_device(
    homolog_features,
    twofold_features,
    twofold_offset_map,
    horizontal_attend_entry_maps,
    horizontal_attend_exit_map,
    vertical_attend_entry_maps,
    vertical_attend_exit_map,
    tensor_product_factors,
    tensor_product_exit_map,
):
    width = lax.axis_size("dap")
    sequences, residues, channels = homolog_features.shape
    rows, _, depth = twofold_features.shape
    heads = twofold_offset_map.shape[1]
    head_size = channels // heads
    groups = channels // LANES
    span = tensor_product_factors.shape[1] // 2
    count = sequences * width
    lanes = max(rows * span, LANES)
    tiles = channels // LANES

    me = lax.axis_index("dap").astype(jnp.int32).reshape(1)

    [halves] = call(
        functools.partial(bias_body, copies=width),
        [((width * heads * rows // 2, residues), BF16, False)],
        [twofold_features, twofold_offset_map.T],
        far=(0, 1),
    )
    features, halves = lax.optimization_barrier((homolog_features, halves))
    own = lax.all_to_all(halves, "dap", split_axis=0, concat_axis=0, tiled=True)
    kept, scores = call(
        functools.partial(row_scores_body, head_size=head_size),
        [
            ((groups, sequences * residues, 3 * LANES), BF16, True),
            ((sequences, groups, residues, LANES // head_size * residues), F32, True),
        ],
        [features, horizontal_attend_entry_maps],
        far=(0, 1),
        flops=10**9,
    )
    own, scores = lax.optimization_barrier((own, scores))
    other = lax.ppermute(own, "dap", [(d, d ^ 1) for d in range(width)])
    bias_scratch = [
        pltpu.VMEM((width * heads * rows // 2, residues), F32),
        pltpu.VMEM((heads // 2, residues, residues), F32),
    ]
    [gated] = call(
        functools.partial(row_first_body, blocks=width, head_size=head_size),
        [((groups // 2, sequences * residues, LANES), BF16, True)],
        [me, own, kept, scores],
        scratch=bias_scratch,
        flops=10**9,
    )
    [sent] = call(
        functools.partial(row_second_body, blocks=width, head_size=head_size),
        [((sequences * residues * tiles, LANES), BF16, True)],
        [me, other, kept, scores, gated, horizontal_attend_exit_map],
        scratch=bias_scratch + [pltpu.VMEM((sequences * residues * tiles, LANES), F32)],
    )
    received = lax.all_to_all(sent, "dap", split_axis=0, concat_axis=0, tiled=True)
    lines, left, right = call(
        functools.partial(column_body, rows=rows, head_size=head_size),
        [
            ((count * rows, channels), F32, True),
            ((lanes, count), BF16, True),
            ((rows * span, count), BF16, True),
        ],
        [received, vertical_attend_entry_maps, vertical_attend_exit_map, tensor_product_factors.T],
        scratch=[
            pltpu.VMEM((count * rows * tiles, LANES), F32),
            pltpu.VMEM((count * rows, 4 * channels), BF16),
            pltpu.VMEM((rows, groups, count, LANES // head_size * count), F32),
            pltpu.VMEM((rows * span, count), F32),
        ],
    )
    [table] = call(
        table_body,
        [((2 * span * span, 2 * depth), BF16, True)],
        [lax.optimization_barrier((tensor_product_exit_map, left))[0]],
        scratch=[pltpu.VMEM((span * span, depth), F32)],
        flops=10**9,
    )
    [alignment] = call(
        functools.partial(arrange_body, rows=rows),
        [((count * rows * tiles, LANES), BF16, False)],
        [lines],
        scratch=[pltpu.VMEM((count * rows * tiles, LANES), F32)],
        flops=10**9,
    )
    pieces, order = gather_blocks(right, (table, alignment))
    radix = len(pieces)
    sizes = dict(order=tuple(order[: width // radix]), radix=radix, span=span, count=count, rows=rows)
    share = residues // radix
    product = pltpu.VMEM((lanes // LANES, width // radix, rows * span, LANES), F32)
    height = rows // 2 * share
    [first] = call(
        functools.partial(outer_first_body, **sizes),
        [((height, 2 * span * span), BF16, True)],
        [me, left, pieces[0]],
        scratch=[product],
        flops=10**9,
    )
    [pair_output] = call(
        functools.partial(outer_last_body, **sizes),
        [(twofold_features.shape, BF16, False)],
        [me, left, *pieces[1:], table, first, twofold_features],
        scratch=[
            product,
            pltpu.VMEM(((radix - 1) * height, 2 * span * span), BF16),
        ],
    )
    alignment = alignment.reshape(count, tiles, rows, LANES).transpose(0, 2, 1, 3)
    return (alignment.reshape(count, rows, channels), pair_output)


def solution(mesh):
    in_specs = (
        P(("crop", "dap"), None, None),
        P(("crop", "dap"), None, None),
        P(),
        P(),
        P(),
        P(),
        P(),
        P(),
        P(),
    )
    out_specs = (P("crop", "dap", None), P(("crop", "dap"), None, None))
    return jax.shard_map(
        per_device, mesh=mesh, in_specs=in_specs, out_specs=out_specs, check_vma=False
    )
```

```python
import functools
import math

import jax
import jax.numpy as jnp
from jax import lax
from jax.experimental import pallas as pl
from jax.experimental.pallas import tpu as pltpu
from jax.sharding import PartitionSpec as P


EPSILON = 1e-05
LANES = 128
F32 = jnp.float32
BF16 = jnp.bfloat16
VMEM = pl.BlockSpec(memory_space=pltpu.VMEM)
SMEM = pl.BlockSpec(memory_space=pltpu.SMEM)


def standardize(values):
    center = values - jnp.mean(values, axis=-1, keepdims=True)
    spread = jnp.mean(center * center, axis=-1, keepdims=True)
    return (center * lax.rsqrt(spread + EPSILON)).astype(BF16)


def dot(left, right):
    return jnp.dot(left, right, preferred_element_type=F32)


def dot_t(left, right):
    return lax.dot_general(left, right, (((1,), (1,)), ((), ())), preferred_element_type=F32)


def call(body, out_shapes, args, scratch=(), limit=16 << 20, flops=0, far=()):
    scalars = [jnp.issubdtype(arg.dtype, jnp.integer) for arg in args]
    return pl.pallas_call(
        body,
        out_shape=[
            pltpu.VMEM(shape, dtype) if near else jax.ShapeDtypeStruct(shape, dtype)
            for shape, dtype, near in out_shapes
        ],
        in_specs=[SMEM if scalar else VMEM for scalar in scalars],
        out_specs=[VMEM] * len(out_shapes),
        scratch_shapes=list(scratch),
        cost_estimate=pl.CostEstimate(flops=flops, bytes_accessed=0, transcendentals=0),
        compiler_params=pltpu.CompilerParams(vmem_limit_bytes=limit),
    )(*[
        arg
        if scalar
        else pltpu.with_memory_space_constraint(arg, pltpu.HBM if at in far else pltpu.VMEM)
        for at, (arg, scalar) in enumerate(zip(args, scalars))
    ])


def lane_masks(width, rows):
    lane = lax.broadcasted_iota(jnp.int32, (rows, LANES), 1)
    return [
        (lane >= start) & (lane < start + width) for start in range(0, LANES, width)
    ]


def masked_rows(block, masks):
    zero = jnp.zeros_like(block)
    return jnp.concatenate([jnp.where(mask, block, zero) for mask in masks], axis=0)


def bias_body(pair_ref, map_ref, out_ref, *, copies):
    rows, _, _ = pair_ref.shape
    heads = map_ref.shape[0]
    height = heads * rows
    row = lax.broadcasted_iota(jnp.int32, (height, heads), 0)
    head = lax.broadcasted_iota(jnp.int32, (height, heads), 1)
    total = None
    for at in range(rows):
        spread = jnp.where(row == head * rows + at, 1.0, 0.0).astype(BF16)
        weights = dot(spread, map_ref[...]).astype(BF16)
        part = dot_t(weights, standardize(pair_ref[at].astype(F32)))
        total = part if total is None else total + part
    block = total.astype(BF16)
    half = height // 2
    for copy in range(copies):
        out_ref[copy * half : (copy + 1) * half, :] = block[copy % 2 * half : (copy % 2 + 1) * half, :]


def scores_of(proj, head_size, masks):
    width = proj.shape[1] // 4
    scale = 1.0 / math.sqrt(head_size)
    scores = []
    for start in range(0, width, LANES):
        queries = proj[:, start : start + LANES]
        keys = masked_rows(proj[:, width + start : width + start + LANES], masks)
        scores.append(dot_t(queries, keys) * scale)
    return scores


def attended_of(scores, values, gates, masks):
    keys = values.shape[0]
    pieces = []
    for at in range(len(masks)):
        piece = scores[at]
        highest = jnp.max(piece, axis=-1, keepdims=True)
        pieces.append(jnp.exp(piece - highest).astype(BF16))
    ones = jnp.ones((keys, LANES), BF16)
    table = jnp.concatenate([masked_rows(values, masks), masked_rows(ones, masks)], axis=1)
    sums = dot(jnp.concatenate(pieces, axis=1), table)
    gate = jax.nn.sigmoid(gates.astype(F32))
    return (gate * (sums[:, :LANES] / sums[:, LANES:])).astype(BF16)


def row_scores_body(features_ref, maps_ref, kept_ref, scores_ref, *, head_size):
    sequences, residues, channels = features_ref.shape
    features = features_ref[...].reshape(sequences * residues, channels)
    proj = dot(standardize(features.astype(F32)), maps_ref[...]).astype(BF16)
    for block, start in enumerate(range(0, channels, LANES)):
        kept_ref[block, :, :LANES] = proj[:, 2 * channels + start : 2 * channels + start + LANES]
        kept_ref[block, :, LANES : 2 * LANES] = proj[:, 3 * channels + start : 3 * channels + start + LANES]
        kept_ref[block, :, 2 * LANES :] = features[:, start : start + LANES]
    masks = lane_masks(head_size, residues)
    for at in range(sequences):
        mine = proj[at * residues : (at + 1) * residues, :]
        for block, scores in enumerate(scores_of(mine, head_size, masks)):
            scores_ref[at, block] = scores


def row_half(bias_ref, kept_ref, scores_ref, wide, bias, first, blocks, head_size):
    sequences, _, residues, _ = scores_ref.shape
    rows = residues // blocks
    heads = bias_ref.shape[0] // residues
    masks = lane_masks(head_size, residues)
    wide[...] = bias_ref[...].astype(F32)
    for source in range(blocks):
        for head in range(heads):
            start = (source * heads + head) * rows
            bias[head, source * rows : (source + 1) * rows, :] = wide[start : start + rows, :]
    gated = []
    for block in range(heads // len(masks)):
        parts = []
        for at in range(sequences):
            mine = pl.ds(at * residues, residues)
            scores = [
                scores_ref[at, first + block, :, k * residues : (k + 1) * residues]
                + bias[block * len(masks) + k]
                for k in range(len(masks))
            ]
            values = kept_ref[first + block, mine, :LANES]
            gates = kept_ref[first + block, mine, LANES : 2 * LANES]
            parts.append(attended_of(scores, values, gates, masks))
        gated.append(parts)
    return gated


def row_first_body(me_ref, bias_ref, kept_ref, scores_ref, out_ref, wide, bias, *, blocks, head_size):
    groups = kept_ref.shape[0] // 2
    residues = scores_ref.shape[2]
    first = jnp.bitwise_and(me_ref[0], 1) * groups
    gated = row_half(bias_ref, kept_ref, scores_ref, wide, bias, first, blocks, head_size)
    for block, parts in enumerate(gated):
        for at, part in enumerate(parts):
            out_ref[block, at * residues : (at + 1) * residues, :] = part


def row_second_body(
    me_ref, bias_ref, kept_ref, scores_ref, gated_ref, exit_ref, out_ref, wide, bias, sent, *, blocks, head_size
):
    groups = kept_ref.shape[0] // 2
    sequences, tiles, residues, _ = scores_ref.shape
    rows = residues // blocks
    parity = jnp.bitwise_and(me_ref[0], 1)
    gated = row_half(bias_ref, kept_ref, scores_ref, wide, bias, (1 - parity) * groups, blocks, head_size)

    def exit_rows(group):
        return exit_ref[pl.ds(pl.multiple_of(group * LANES, LANES), LANES), :]

    for at in range(sequences):
        mine = slice(at * residues, (at + 1) * residues)
        delta = None
        for block in range(groups):
            for part, group in (
                (gated_ref[block, mine, :], parity * groups + block),
                (gated[block][at], (1 - parity) * groups + block),
            ):
                more = dot(part, exit_rows(group))
                delta = more if delta is None else delta + more
        for tile in range(tiles):
            line = kept_ref[tile, mine, 2 * LANES :].astype(F32) + delta[:, tile * LANES : (tile + 1) * LANES]
            for target in range(blocks):
                start = ((target * sequences + at) * tiles + tile) * rows
                sent[start : start + rows, :] = line[target * rows : (target + 1) * rows, :]
    out_ref[...] = sent[...].astype(BF16)


def column_body(
    received_ref, maps_ref, exit_ref, factors_ref, lines_ref, left_ref, right_ref, wide, proj_ref, score_ref, turned,
    *, rows, head_size
):
    channels = maps_ref.shape[0]
    tiles = channels // LANES
    sequences = received_ref.shape[0] // (rows * tiles)
    span = factors_ref.shape[0] // 2
    wide[...] = received_ref[...].astype(F32)
    if left_ref.shape[0] > rows * span:
        left_ref[...] = jnp.zeros_like(left_ref)
    masks = lane_masks(head_size, sequences)
    chosen = [
        [pl.ds(tile * rows + at, sequences, stride=tiles * rows) for tile in range(tiles)]
        for at in range(rows)
    ]
    lines = jnp.concatenate(
        [jnp.concatenate([wide[rows_of, :] for rows_of in one], axis=1) for one in chosen], axis=0
    )
    proj_ref[...] = dot(standardize(lines), maps_ref[...]).astype(BF16)
    for at in range(rows):
        proj = proj_ref[at * sequences : (at + 1) * sequences, :]
        for block, scores in enumerate(scores_of(proj, head_size, masks)):
            score_ref[at, block] = scores
    gated = []
    for at in range(rows):
        mine = slice(at * sequences, (at + 1) * sequences)
        parts = []
        for block, start in enumerate(range(0, channels, LANES)):
            scores = [
                score_ref[at, block, :, k * sequences : (k + 1) * sequences] for k in range(len(masks))
            ]
            values = proj_ref[mine, 2 * channels + start : 2 * channels + start + LANES]
            gates = proj_ref[mine, 3 * channels + start : 3 * channels + start + LANES]
            parts.append(attended_of(scores, values, gates, masks))
        gated.append(jnp.concatenate(parts, axis=1))
    lines = lines + dot(jnp.concatenate(gated, axis=0), exit_ref[...])
    lines = lines.astype(BF16).astype(F32)
    lines_ref[...] = lines
    factors = dot_t(factors_ref[...], standardize(lines))
    for at in range(rows):
        mine = slice(at * sequences, (at + 1) * sequences)
        left_ref[at * span : (at + 1) * span, :] = factors[:span, mine].astype(BF16)
        turned[pl.ds(at, span, stride=rows), :] = factors[span:, mine]
    right_ref[...] = turned[...].astype(BF16)


def arrange_body(lines_ref, out_ref, done, *, rows):
    total, channels = lines_ref.shape
    sequences = total // rows
    tiles = channels // LANES
    for at in range(rows):
        for tile in range(tiles):
            done[pl.ds(tile * rows + at, sequences, stride=tiles * rows), :] = lines_ref[
                at * sequences : (at + 1) * sequences, tile * LANES : (tile + 1) * LANES
            ]
    out_ref[...] = done[...].astype(BF16)


def table_body(exit_ref, out_ref, wide):
    depth = exit_ref.shape[1]
    span = math.isqrt(exit_ref.shape[0])
    wide[...] = exit_ref[...].astype(F32)
    zero = jnp.zeros((span, depth), BF16)
    for e in range(span):
        weights = wide[pl.ds(e, span, stride=span), :].astype(BF16)
        for row, side in enumerate(([weights, zero], [zero, weights])):
            start = (2 * e + row) * span
            out_ref[start : start + span, :] = jnp.concatenate(side, axis=1)


def outer_rows(left_ref, right_refs, out_ref, product, order, span, count, rows):
    width = rows * span
    lanes = left_ref.shape[0]
    residues = len(order) * rows
    left = left_ref[...]
    zero = jnp.zeros_like(left)
    both = jnp.concatenate(
        [jnp.concatenate([left, zero], axis=1), jnp.concatenate([zero, left], axis=1)], axis=0
    )
    half = len(order) // 2
    lane = lax.broadcasted_iota(jnp.int32, (residues, LANES), 1)
    for piece, right_ref in enumerate(right_refs):
        products = dot_t(
            jnp.concatenate([right_ref[: half * width, :], right_ref[half * width :, :]], axis=1), both
        ) * (1.0 / count)
        for at in range(len(order)):
            start = at % half * width
            side = at // half * lanes
            for tile in range(lanes // LANES):
                product[tile, at] = products[
                    start : start + width, side + tile * LANES : side + (tile + 1) * LANES
                ]
        for e in range(0, span, 2):
            for tile in range(lanes // LANES):
                halves = couple_of(product, tile, e, rows, residues)
                swapped = [pltpu.roll(part, LANES // 2, 1) for part in halves]
                for pair in range(2 * tile, min(2 * tile + 2, rows // 2)):
                    low, high = (halves[0], swapped[1]) if pair % 2 == 0 else (swapped[0], halves[1])
                    start = (piece * (rows // 2) + pair) * residues
                    out_ref[start : start + residues, e // 2 * LANES : (e // 2 + 1) * LANES] = jnp.where(
                        lane < LANES // 2, low, high
                    ).astype(BF16)


def couple_of(product, tile, e, rows, residues):
    if rows % 8 == 0:
        return [
            product[tile, :, (e + odd) * rows : (e + odd + 1) * rows, :].reshape(residues, LANES)
            for odd in (0, 1)
        ]
    couples = product[tile, :, e * rows : (e + 2) * rows, :]
    sources = couples.shape[0]
    if rows != 4:
        return [
            jnp.concatenate([couples[at, odd * rows : (odd + 1) * rows] for at in range(sources)], axis=0)
            for odd in (0, 1)
        ]
    couples = couples.reshape(sources // 2, 2, 2 * rows, LANES)
    first, second = couples[:, 0], couples[:, 1]
    upper = lax.broadcasted_iota(jnp.int32, first.shape, 1) < rows
    even = jnp.where(upper, first, pltpu.roll(second, rows, 1))
    odd = jnp.where(upper, pltpu.roll(first, rows, 1), second)
    return [part.reshape(residues, LANES) for part in (even, odd)]


def outer_first_body(left_ref, right_ref, out_ref, product, **sizes):
    outer_rows(left_ref, [right_ref], out_ref, product, **sizes)


def outer_last_body(me_ref, left_ref, *refs, radix, order, rows, **sizes):
    right_refs = refs[: radix - 1]
    table_ref, first_ref, pair_ref, out_ref, product, rest, stage = refs[radix - 1 :]
    depth = pair_ref.shape[2]
    outer_rows(left_ref, right_refs, rest, product, order=order, rows=rows, **sizes)
    delta = dot(jnp.concatenate([first_ref[...], rest[...]], axis=0), table_ref[...])
    height = first_ref.shape[0]
    residues = height // (rows // 2)
    digit = me_ref[0] % radix
    mine = me_ref[0] // radix
    places = []
    for place in range(radix):
        value = delta[:height]
        for piece in range(1, radix):
            value = jnp.where(
                jnp.bitwise_xor(digit, piece) == place, delta[piece * height : (piece + 1) * height], value
            )
        places.append(value)
    group = rows * radix
    for row in range(rows):
        block = slice((row // 2) * residues, (row // 2 + 1) * residues)
        side = slice((row % 2) * depth, (row % 2 + 1) * depth)
        more = interleave([value[block, side] for value in places], rows)
        for at, step in enumerate(order):
            source = jnp.bitwise_xor(mine, step // radix)
            to = pl.ds(pl.multiple_of(source * group, group), group)
            stage[row, to, :] = more[at * group : (at + 1) * group]
        out_ref[row] = (pair_ref[row].astype(F32) + stage[row]).astype(BF16)


def interleave(parts, rows):
    total, lanes = parts[0].shape
    if rows != 4 or len(parts) != 2:
        return jnp.concatenate(
            [part[at : at + rows] for at in range(0, total, rows) for part in parts], axis=0
        )
    first, second = [part.reshape(total // 8, 8, lanes) for part in parts]
    upper = lax.broadcasted_iota(jnp.int32, first.shape, 1) < rows
    even = jnp.where(upper, first, pltpu.roll(second, rows, 1))
    odd = jnp.where(upper, pltpu.roll(first, rows, 1), second)
    return jnp.concatenate([even[:, None], odd[:, None]], axis=1).reshape(2 * total, lanes)


def gather_rounds(width):
    rounds = []
    stride = width
    while stride > 1:
        radix = 4 if stride % 4 == 0 else 2
        stride //= radix
        rounds.append([step * stride for step in reversed(range(1, radix))])
    return rounds


def gather_blocks(block, beside=()):
    width = lax.axis_size("dap")
    pieces = [block]
    order = [0]
    for at, steps in enumerate(gather_rounds(width)):
        stacked = jnp.concatenate(pieces, axis=0) if len(pieces) > 1 else pieces[0]
        if 0 < at <= len(beside):
            stacked, _ = lax.optimization_barrier((stacked, beside[at - 1]))
        pieces = [stacked]
        for step in steps:
            pieces.append(lax.ppermute(stacked, "dap", [(d, d ^ step) for d in range(width)]))
        order = order + [k ^ step for step in steps for k in order]
    return pieces, order


def per_device(
    homolog_features,
    twofold_features,
    twofold_offset_map,
    horizontal_attend_entry_maps,
    horizontal_attend_exit_map,
    vertical_attend_entry_maps,
    vertical_attend_exit_map,
    tensor_product_factors,
    tensor_product_exit_map,
):
    width = lax.axis_size("dap")
    sequences, residues, channels = homolog_features.shape
    rows, _, depth = twofold_features.shape
    heads = twofold_offset_map.shape[1]
    head_size = channels // heads
    groups = channels // LANES
    span = tensor_product_factors.shape[1] // 2
    count = sequences * width
    lanes = max(rows * span, LANES)
    tiles = channels // LANES

    me = lax.axis_index("dap").astype(jnp.int32).reshape(1)

    [halves] = call(
        functools.partial(bias_body, copies=width),
        [((width * heads * rows // 2, residues), BF16, False)],
        [twofold_features, twofold_offset_map.T],
        far=(0, 1),
    )
    features, halves = lax.optimization_barrier((homolog_features, halves))
    own = lax.all_to_all(halves, "dap", split_axis=0, concat_axis=0, tiled=True)
    kept, scores = call(
        functools.partial(row_scores_body, head_size=head_size),
        [
            ((groups, sequences * residues, 3 * LANES), BF16, True),
            ((sequences, groups, residues, LANES // head_size * residues), F32, True),
        ],
        [features, horizontal_attend_entry_maps],
        far=(0, 1),
        flops=10**9,
    )
    own, scores = lax.optimization_barrier((own, scores))
    other = lax.ppermute(own, "dap", [(d, d ^ 1) for d in range(width)])
    bias_scratch = [
        pltpu.VMEM((width * heads * rows // 2, residues), F32),
        pltpu.VMEM((heads // 2, residues, residues), F32),
    ]
    [gated] = call(
        functools.partial(row_first_body, blocks=width, head_size=head_size),
        [((groups // 2, sequences * residues, LANES), BF16, True)],
        [me, own, kept, scores],
        scratch=bias_scratch,
        flops=10**9,
    )
    [sent] = call(
        functools.partial(row_second_body, blocks=width, head_size=head_size),
        [((sequences * residues * tiles, LANES), BF16, True)],
        [me, other, kept, scores, gated, horizontal_attend_exit_map],
        scratch=bias_scratch + [pltpu.VMEM((sequences * residues * tiles, LANES), F32)],
    )
    received = lax.all_to_all(sent, "dap", split_axis=0, concat_axis=0, tiled=True)
    lines, left, right = call(
        functools.partial(column_body, rows=rows, head_size=head_size),
        [
            ((count * rows, channels), F32, True),
            ((lanes, count), BF16, True),
            ((rows * span, count), BF16, True),
        ],
        [received, vertical_attend_entry_maps, vertical_attend_exit_map, tensor_product_factors.T],
        scratch=[
            pltpu.VMEM((count * rows * tiles, LANES), F32),
            pltpu.VMEM((count * rows, 4 * channels), BF16),
            pltpu.VMEM((rows, groups, count, LANES // head_size * count), F32),
            pltpu.VMEM((rows * span, count), F32),
        ],
    )
    [table] = call(
        table_body,
        [((2 * span * span, 2 * depth), BF16, True)],
        [lax.optimization_barrier((tensor_product_exit_map, left))[0]],
        scratch=[pltpu.VMEM((span * span, depth), F32)],
        flops=10**9,
    )
    [alignment] = call(
        functools.partial(arrange_body, rows=rows),
        [((count * rows * tiles, LANES), BF16, False)],
        [lines],
        scratch=[pltpu.VMEM((count * rows * tiles, LANES), F32)],
        flops=10**9,
    )
    pieces, order = gather_blocks(right, (table, alignment))
    radix = len(pieces)
    sizes = dict(order=tuple(order[: width // radix]), span=span, count=count, rows=rows)
    share = residues // radix
    product = pltpu.VMEM((lanes // LANES, width // radix, rows * span, LANES), F32)
    height = rows // 2 * share
    [first] = call(
        functools.partial(outer_first_body, **sizes),
        [((height, 2 * span * span), BF16, True)],
        [left, pieces[0]],
        scratch=[product],
        flops=10**9,
    )
    [pair_output] = call(
        functools.partial(outer_last_body, radix=radix, **sizes),
        [(twofold_features.shape, BF16, False)],
        [me, left, *pieces[1:], table, first, twofold_features],
        scratch=[
            product,
            pltpu.VMEM(((radix - 1) * height, 2 * span * span), BF16),
            pltpu.VMEM((rows, residues, depth), F32),
        ],
    )
    alignment = alignment.reshape(count, tiles, rows, LANES).transpose(0, 2, 1, 3)
    return (alignment.reshape(count, rows, channels), pair_output)


def solution(mesh):
    in_specs = (
        P(("crop", "dap"), None, None),
        P(("crop", "dap"), None, None),
        P(),
        P(),
        P(),
        P(),
        P(),
        P(),
        P(),
    )
    out_specs = (P("crop", "dap", None), P(("crop", "dap"), None, None))
    return jax.shard_map(
        per_device, mesh=mesh, in_specs=in_specs, out_specs=out_specs, check_vma=False
    )
```

```python
import functools
import math

import jax
import jax.numpy as jnp
from jax import lax
from jax.experimental import pallas as pl
from jax.experimental.pallas import tpu as pltpu
from jax.sharding import PartitionSpec as P


EPSILON = 1e-05
LANES = 128
LOG2_E = math.log2(math.e)
F32 = jnp.float32
BF16 = jnp.bfloat16
VMEM = pl.BlockSpec(memory_space=pltpu.VMEM)
SMEM = pl.BlockSpec(memory_space=pltpu.SMEM)


def standardize(values):
    center = values - jnp.mean(values, axis=-1, keepdims=True)
    spread = jnp.mean(center * center, axis=-1, keepdims=True)
    return (center * lax.rsqrt(spread + EPSILON)).astype(BF16)


def dot(left, right):
    return jnp.dot(left, right, preferred_element_type=F32)


def dot_t(left, right):
    return lax.dot_general(left, right, (((1,), (1,)), ((), ())), preferred_element_type=F32)


def call(body, out_shapes, args, scratch=(), limit=16 << 20, flops=0, far=()):
    scalars = [jnp.issubdtype(arg.dtype, jnp.integer) for arg in args]
    return pl.pallas_call(
        body,
        out_shape=[
            pltpu.VMEM(shape, dtype) if near else jax.ShapeDtypeStruct(shape, dtype)
            for shape, dtype, near in out_shapes
        ],
        in_specs=[SMEM if scalar else VMEM for scalar in scalars],
        out_specs=[VMEM] * len(out_shapes),
        scratch_shapes=list(scratch),
        cost_estimate=pl.CostEstimate(flops=flops, bytes_accessed=0, transcendentals=0),
        compiler_params=pltpu.CompilerParams(vmem_limit_bytes=limit),
    )(*[
        arg
        if scalar
        else pltpu.with_memory_space_constraint(arg, pltpu.HBM if at in far else pltpu.VMEM)
        for at, (arg, scalar) in enumerate(zip(args, scalars))
    ])


def lane_masks(width, rows):
    lane = lax.broadcasted_iota(jnp.int32, (rows, LANES), 1)
    return [
        (lane >= start) & (lane < start + width) for start in range(0, LANES, width)
    ]


def masked_rows(block, masks):
    zero = jnp.zeros_like(block)
    return jnp.concatenate([jnp.where(mask, block, zero) for mask in masks], axis=0)


def bias_body(pair_ref, map_ref, out_ref, *, copies):
    rows, _, _ = pair_ref.shape
    heads = map_ref.shape[0]
    height = heads * rows
    row = lax.broadcasted_iota(jnp.int32, (height, heads), 0)
    head = lax.broadcasted_iota(jnp.int32, (height, heads), 1)
    total = None
    for at in range(rows):
        spread = jnp.where(row == head * rows + at, 1.0, 0.0).astype(BF16)
        weights = dot(spread, map_ref[...]).astype(BF16)
        part = dot_t(weights, standardize(pair_ref[at].astype(F32)))
        total = part if total is None else total + part
    block = total.astype(BF16)
    half = height // 2
    for copy in range(copies):
        out_ref[copy * half : (copy + 1) * half, :] = block[copy % 2 * half : (copy % 2 + 1) * half, :]


def project(values, maps, head_size):
    width = maps.shape[1] // 4
    proj = dot(standardize(values), maps)
    queries = proj[:, :width] * (LOG2_E / math.sqrt(head_size))
    return jnp.concatenate([queries, proj[:, width:]], axis=1).astype(BF16)


def scores_of(proj, masks):
    width = proj.shape[1] // 4
    scores = []
    for start in range(0, width, LANES):
        queries = proj[:, start : start + LANES]
        keys = masked_rows(proj[:, width + start : width + start + LANES], masks)
        scores.append(dot_t(queries, keys))
    return scores


def attended_of(scores, values, gates, masks):
    keys = values.shape[0]
    pieces = []
    for at in range(len(masks)):
        piece = scores[at]
        highest = jnp.max(piece, axis=-1, keepdims=True)
        pieces.append(jnp.exp2(piece - highest).astype(BF16))
    ones = jnp.ones((keys, LANES), BF16)
    table = jnp.concatenate([masked_rows(values, masks), masked_rows(ones, masks)], axis=1)
    sums = dot(jnp.concatenate(pieces, axis=1), table)
    gate = jax.nn.sigmoid(gates.astype(F32))
    return (gate * (sums[:, :LANES] / sums[:, LANES:])).astype(BF16)


def row_scores_body(features_ref, maps_ref, kept_ref, scores_ref, *, head_size):
    sequences, residues, channels = features_ref.shape
    features = features_ref[...].reshape(sequences * residues, channels)
    proj = project(features.astype(F32), maps_ref[...], head_size)
    for block, start in enumerate(range(0, channels, LANES)):
        kept_ref[block, :, :LANES] = proj[:, 2 * channels + start : 2 * channels + start + LANES]
        kept_ref[block, :, LANES : 2 * LANES] = proj[:, 3 * channels + start : 3 * channels + start + LANES]
        kept_ref[block, :, 2 * LANES :] = features[:, start : start + LANES]
    masks = lane_masks(head_size, residues)
    for at in range(sequences):
        mine = proj[at * residues : (at + 1) * residues, :]
        for block, scores in enumerate(scores_of(mine, masks)):
            scores_ref[at, block] = scores


def row_half(bias_ref, kept_ref, scores_ref, wide, bias, first, blocks, head_size):
    sequences, _, residues, _ = scores_ref.shape
    rows = residues // blocks
    heads = bias_ref.shape[0] // residues
    masks = lane_masks(head_size, residues)
    wide[...] = bias_ref[...].astype(F32) * LOG2_E
    for source in range(blocks):
        for head in range(heads):
            start = (source * heads + head) * rows
            bias[head, source * rows : (source + 1) * rows, :] = wide[start : start + rows, :]
    gated = []
    for block in range(heads // len(masks)):
        parts = []
        for at in range(sequences):
            mine = pl.ds(at * residues, residues)
            scores = [
                scores_ref[at, first + block, :, k * residues : (k + 1) * residues]
                + bias[block * len(masks) + k]
                for k in range(len(masks))
            ]
            values = kept_ref[first + block, mine, :LANES]
            gates = kept_ref[first + block, mine, LANES : 2 * LANES]
            parts.append(attended_of(scores, values, gates, masks))
        gated.append(parts)
    return gated


def exit_share(gated, exit_ref, first, at):
    delta = None
    for block, parts in enumerate(gated):
        rows = pl.ds(pl.multiple_of((first + block) * LANES, LANES), LANES)
        more = dot(parts[at], exit_ref[rows, :])
        delta = more if delta is None else delta + more
    return delta


def row_first_body(me_ref, bias_ref, kept_ref, scores_ref, exit_ref, out_ref, wide, bias, *, blocks, head_size):
    sequences, tiles, residues, _ = scores_ref.shape
    first = jnp.bitwise_and(me_ref[0], 1) * (tiles // 2)
    gated = row_half(bias_ref, kept_ref, scores_ref, wide, bias, first, blocks, head_size)
    for at in range(sequences):
        mine = slice(at * residues, (at + 1) * residues)
        delta = exit_share(gated, exit_ref, first, at)
        for tile in range(tiles):
            side = slice(tile * LANES, (tile + 1) * LANES)
            out_ref[mine, side] = kept_ref[tile, mine, 2 * LANES :].astype(F32) + delta[:, side]


def row_second_body(
    me_ref, bias_ref, kept_ref, scores_ref, exit_ref, lines_ref, out_ref, wide, bias, sent, *, blocks, head_size
):
    sequences, tiles, residues, _ = scores_ref.shape
    rows = residues // blocks
    first = (1 - jnp.bitwise_and(me_ref[0], 1)) * (tiles // 2)
    gated = row_half(bias_ref, kept_ref, scores_ref, wide, bias, first, blocks, head_size)
    for at in range(sequences):
        line = lines_ref[at * residues : (at + 1) * residues, :] + exit_share(gated, exit_ref, first, at)
        for tile in range(tiles):
            for target in range(blocks):
                start = ((target * sequences + at) * tiles + tile) * rows
                sent[start : start + rows, :] = line[
                    target * rows : (target + 1) * rows, tile * LANES : (tile + 1) * LANES
                ]
    out_ref[...] = sent[...].astype(BF16)


def column_body(
    received_ref, maps_ref, exit_ref, factors_ref, lines_ref, left_ref, right_ref, wide, proj_ref, score_ref, turned,
    *, rows, head_size
):
    channels = maps_ref.shape[0]
    tiles = channels // LANES
    sequences = received_ref.shape[0] // (rows * tiles)
    span = factors_ref.shape[0] // 2
    wide[...] = received_ref[...].astype(F32)
    if left_ref.shape[0] > rows * span:
        left_ref[...] = jnp.zeros_like(left_ref)
    masks = lane_masks(head_size, sequences)
    chosen = [
        [pl.ds(tile * rows + at, sequences, stride=tiles * rows) for tile in range(tiles)]
        for at in range(rows)
    ]
    lines = jnp.concatenate(
        [jnp.concatenate([wide[rows_of, :] for rows_of in one], axis=1) for one in chosen], axis=0
    )
    proj_ref[...] = project(lines, maps_ref[...], head_size)
    for at in range(rows):
        proj = proj_ref[at * sequences : (at + 1) * sequences, :]
        for block, scores in enumerate(scores_of(proj, masks)):
            score_ref[at, block] = scores
    gated = []
    for at in range(rows):
        mine = slice(at * sequences, (at + 1) * sequences)
        parts = []
        for block, start in enumerate(range(0, channels, LANES)):
            scores = [
                score_ref[at, block, :, k * sequences : (k + 1) * sequences] for k in range(len(masks))
            ]
            values = proj_ref[mine, 2 * channels + start : 2 * channels + start + LANES]
            gates = proj_ref[mine, 3 * channels + start : 3 * channels + start + LANES]
            parts.append(attended_of(scores, values, gates, masks))
        gated.append(jnp.concatenate(parts, axis=1))
    lines = lines + dot(jnp.concatenate(gated, axis=0), exit_ref[...])
    lines = lines.astype(BF16).astype(F32)
    lines_ref[...] = lines
    factors = dot_t(factors_ref[...], standardize(lines))
    for at in range(rows):
        mine = slice(at * sequences, (at + 1) * sequences)
        left_ref[at * span : (at + 1) * span, :] = factors[:span, mine].astype(BF16)
        turned[pl.ds(at, span, stride=rows), :] = factors[span:, mine]
    right_ref[...] = turned[...].astype(BF16)


def arrange_body(lines_ref, out_ref, done, *, rows):
    total, channels = lines_ref.shape
    sequences = total // rows
    tiles = channels // LANES
    for at in range(rows):
        for tile in range(tiles):
            done[pl.ds(tile * rows + at, sequences, stride=tiles * rows), :] = lines_ref[
                at * sequences : (at + 1) * sequences, tile * LANES : (tile + 1) * LANES
            ]
    out_ref[...] = done[...].astype(BF16)


def table_body(exit_ref, out_ref, wide):
    depth = exit_ref.shape[1]
    span = math.isqrt(exit_ref.shape[0])
    wide[...] = exit_ref[...].astype(F32)
    zero = jnp.zeros((span, depth), BF16)
    for e in range(span):
        weights = wide[pl.ds(e, span, stride=span), :].astype(BF16)
        for row, side in enumerate(([weights, zero], [zero, weights])):
            start = (2 * e + row) * span
            out_ref[start : start + span, :] = jnp.concatenate(side, axis=1)


def outer_rows(left_ref, right_refs, out_ref, product, order, span, count, rows):
    width = rows * span
    lanes = left_ref.shape[0]
    residues = len(order) * rows
    left = left_ref[...]
    zero = jnp.zeros_like(left)
    both = jnp.concatenate(
        [jnp.concatenate([left, zero], axis=1), jnp.concatenate([zero, left], axis=1)], axis=0
    )
    half = len(order) // 2
    lane = lax.broadcasted_iota(jnp.int32, (residues, LANES), 1)
    for piece, right_ref in enumerate(right_refs):
        products = dot_t(
            jnp.concatenate([right_ref[: half * width, :], right_ref[half * width :, :]], axis=1), both
        ) * (1.0 / count)
        for at in range(len(order)):
            start = at % half * width
            side = at // half * lanes
            for tile in range(lanes // LANES):
                product[tile, at] = products[
                    start : start + width, side + tile * LANES : side + (tile + 1) * LANES
                ]
        for e in range(0, span, 2):
            for tile in range(lanes // LANES):
                halves = couple_of(product, tile, e, rows, residues)
                swapped = [pltpu.roll(part, LANES // 2, 1) for part in halves]
                for pair in range(2 * tile, min(2 * tile + 2, rows // 2)):
                    low, high = (halves[0], swapped[1]) if pair % 2 == 0 else (swapped[0], halves[1])
                    start = (piece * (rows // 2) + pair) * residues
                    out_ref[start : start + residues, e // 2 * LANES : (e // 2 + 1) * LANES] = jnp.where(
                        lane < LANES // 2, low, high
                    ).astype(BF16)


def couple_of(product, tile, e, rows, residues):
    if rows % 8 == 0:
        return [
            product[tile, :, (e + odd) * rows : (e + odd + 1) * rows, :].reshape(residues, LANES)
            for odd in (0, 1)
        ]
    couples = product[tile, :, e * rows : (e + 2) * rows, :]
    sources = couples.shape[0]
    if rows != 4:
        return [
            jnp.concatenate([couples[at, odd * rows : (odd + 1) * rows] for at in range(sources)], axis=0)
            for odd in (0, 1)
        ]
    couples = couples.reshape(sources // 2, 2, 2 * rows, LANES)
    first, second = couples[:, 0], couples[:, 1]
    upper = lax.broadcasted_iota(jnp.int32, first.shape, 1) < rows
    even = jnp.where(upper, first, pltpu.roll(second, rows, 1))
    odd = jnp.where(upper, pltpu.roll(first, rows, 1), second)
    return [part.reshape(residues, LANES) for part in (even, odd)]


def outer_first_body(left_ref, right_ref, out_ref, product, **sizes):
    outer_rows(left_ref, [right_ref], out_ref, product, **sizes)


def outer_last_body(me_ref, left_ref, *refs, radix, order, rows, **sizes):
    right_refs = refs[: radix - 1]
    table_ref, first_ref, pair_ref, out_ref, product, rest, stage = refs[radix - 1 :]
    depth = pair_ref.shape[2]
    outer_rows(left_ref, right_refs, rest, product, order=order, rows=rows, **sizes)
    delta = dot(jnp.concatenate([first_ref[...], rest[...]], axis=0), table_ref[...])
    height = first_ref.shape[0]
    residues = height // (rows // 2)
    digit = me_ref[0] % radix
    mine = me_ref[0] // radix
    places = []
    for place in range(radix):
        value = delta[:height]
        for piece in range(1, radix):
            value = jnp.where(
                jnp.bitwise_xor(digit, piece) == place, delta[piece * height : (piece + 1) * height], value
            )
        places.append(value)
    group = rows * radix
    for row in range(rows):
        block = slice((row // 2) * residues, (row // 2 + 1) * residues)
        side = slice((row % 2) * depth, (row % 2 + 1) * depth)
        more = interleave([value[block, side] for value in places], rows)
        for at, step in enumerate(order):
            source = jnp.bitwise_xor(mine, step // radix)
            to = pl.ds(pl.multiple_of(source * group, group), group)
            stage[row, to, :] = more[at * group : (at + 1) * group]
        out_ref[row] = (pair_ref[row].astype(F32) + stage[row]).astype(BF16)


def interleave(parts, rows):
    total, lanes = parts[0].shape
    if rows != 4 or len(parts) != 2:
        return jnp.concatenate(
            [part[at : at + rows] for at in range(0, total, rows) for part in parts], axis=0
        )
    first, second = [part.reshape(total // 8, 8, lanes) for part in parts]
    upper = lax.broadcasted_iota(jnp.int32, first.shape, 1) < rows
    even = jnp.where(upper, first, pltpu.roll(second, rows, 1))
    odd = jnp.where(upper, pltpu.roll(first, rows, 1), second)
    return jnp.concatenate([even[:, None], odd[:, None]], axis=1).reshape(2 * total, lanes)


def gather_rounds(width):
    rounds = []
    stride = width
    while stride > 1:
        radix = 4 if stride % 4 == 0 else 2
        stride //= radix
        rounds.append([step * stride for step in reversed(range(1, radix))])
    return rounds


def gather_blocks(block, beside=()):
    width = lax.axis_size("dap")
    pieces = [block]
    order = [0]
    for at, steps in enumerate(gather_rounds(width)):
        stacked = jnp.concatenate(pieces, axis=0) if len(pieces) > 1 else pieces[0]
        if 0 < at <= len(beside):
            stacked, _ = lax.optimization_barrier((stacked, beside[at - 1]))
        pieces = [stacked]
        for step in steps:
            pieces.append(lax.ppermute(stacked, "dap", [(d, d ^ step) for d in range(width)]))
        order = order + [k ^ step for step in steps for k in order]
    return pieces, order


def per_device(
    homolog_features,
    twofold_features,
    twofold_offset_map,
    horizontal_attend_entry_maps,
    horizontal_attend_exit_map,
    vertical_attend_entry_maps,
    vertical_attend_exit_map,
    tensor_product_factors,
    tensor_product_exit_map,
):
    width = lax.axis_size("dap")
    sequences, residues, channels = homolog_features.shape
    rows, _, depth = twofold_features.shape
    heads = twofold_offset_map.shape[1]
    head_size = channels // heads
    groups = channels // LANES
    span = tensor_product_factors.shape[1] // 2
    count = sequences * width
    lanes = max(rows * span, LANES)
    tiles = channels // LANES

    me = lax.axis_index("dap").astype(jnp.int32).reshape(1)

    [halves] = call(
        functools.partial(bias_body, copies=width),
        [((width * heads * rows // 2, residues), BF16, False)],
        [twofold_features, twofold_offset_map.T],
        far=(0, 1),
    )
    features, halves = lax.optimization_barrier((homolog_features, halves))
    own = lax.all_to_all(halves, "dap", split_axis=0, concat_axis=0, tiled=True)
    kept, scores = call(
        functools.partial(row_scores_body, head_size=head_size),
        [
            ((groups, sequences * residues, 3 * LANES), BF16, True),
            ((sequences, groups, residues, LANES // head_size * residues), F32, True),
        ],
        [features, horizontal_attend_entry_maps],
        far=(0, 1),
        flops=10**9,
    )
    own, scores = lax.optimization_barrier((own, scores))
    other = lax.ppermute(own, "dap", [(d, d ^ 1) for d in range(width)])
    bias_scratch = [
        pltpu.VMEM((width * heads * rows // 2, residues), F32),
        pltpu.VMEM((heads // 2, residues, residues), F32),
    ]
    [lines] = call(
        functools.partial(row_first_body, blocks=width, head_size=head_size),
        [((sequences * residues, channels), F32, True)],
        [me, own, kept, scores, horizontal_attend_exit_map],
        scratch=bias_scratch,
        flops=10**9,
    )
    [sent] = call(
        functools.partial(row_second_body, blocks=width, head_size=head_size),
        [((sequences * residues * tiles, LANES), BF16, True)],
        [me, other, kept, scores, horizontal_attend_exit_map, lines],
        scratch=bias_scratch + [pltpu.VMEM((sequences * residues * tiles, LANES), F32)],
    )
    received = lax.all_to_all(sent, "dap", split_axis=0, concat_axis=0, tiled=True)
    lines, left, right = call(
        functools.partial(column_body, rows=rows, head_size=head_size),
        [
            ((count * rows, channels), F32, True),
            ((lanes, count), BF16, True),
            ((rows * span, count), BF16, True),
        ],
        [received, vertical_attend_entry_maps, vertical_attend_exit_map, tensor_product_factors.T],
        scratch=[
            pltpu.VMEM((count * rows * tiles, LANES), F32),
            pltpu.VMEM((count * rows, 4 * channels), BF16),
            pltpu.VMEM((rows, groups, count, LANES // head_size * count), F32),
            pltpu.VMEM((rows * span, count), F32),
        ],
    )
    [table] = call(
        table_body,
        [((2 * span * span, 2 * depth), BF16, True)],
        [lax.optimization_barrier((tensor_product_exit_map, left))[0]],
        scratch=[pltpu.VMEM((span * span, depth), F32)],
        flops=10**9,
    )
    [alignment] = call(
        functools.partial(arrange_body, rows=rows),
        [((count * rows * tiles, LANES), BF16, False)],
        [lines],
        scratch=[pltpu.VMEM((count * rows * tiles, LANES), F32)],
        flops=10**9,
    )
    pieces, order = gather_blocks(right, (table, alignment))
    radix = len(pieces)
    sizes = dict(order=tuple(order[: width // radix]), span=span, count=count, rows=rows)
    share = residues // radix
    product = pltpu.VMEM((lanes // LANES, width // radix, rows * span, LANES), F32)
    height = rows // 2 * share
    [first] = call(
        functools.partial(outer_first_body, **sizes),
        [((height, 2 * span * span), BF16, True)],
        [left, pieces[0]],
        scratch=[product],
        flops=10**9,
    )
    [pair_output] = call(
        functools.partial(outer_last_body, radix=radix, **sizes),
        [(twofold_features.shape, BF16, False)],
        [me, left, *pieces[1:], table, first, twofold_features],
        scratch=[
            product,
            pltpu.VMEM(((radix - 1) * height, 2 * span * span), BF16),
            pltpu.VMEM((rows, residues, depth), F32),
        ],
    )
    alignment = alignment.reshape(count, tiles, rows, LANES).transpose(0, 2, 1, 3)
    return (alignment.reshape(count, rows, channels), pair_output)


def solution(mesh):
    in_specs = (
        P(("crop", "dap"), None, None),
        P(("crop", "dap"), None, None),
        P(),
        P(),
        P(),
        P(),
        P(),
        P(),
        P(),
    )
    out_specs = (P("crop", "dap", None), P(("crop", "dap"), None, None))
    return jax.shard_map(
        per_device, mesh=mesh, in_specs=in_specs, out_specs=out_specs, check_vma=False
    )
```
